256 devices in a mesh: dp: 2 (over y_lo), seq: 32 (over z, y_hi, core), chan: 4 (over x).
Axes of the slice: x: 4, y: 4 (y_hi: 2, y_lo: 2; y = y_hi * 2 + y_lo), z: 8, core: 2. Of those that a mesh axis runs over, the one named last changes fastest.
Arguments:
- layer_input: bfloat16 [2, 4096, 2560], P('dp', ('seq', 'chan')), may hold values from -24 to 24
- inner_weight: bfloat16 [2560, 2560], P(None, 'chan'), may hold values from -0.125 to 0.125
- mixer_weight: bfloat16 [2560, 256], replicated, may hold values from -0.01171875 to 0.01171875
- step_weight: bfloat16 [2560, 40], P(None, 'chan'), may hold values from -0.125 to 0.125
- conv_inner: float32 [4, 2560], P(None, 'chan'), may hold values from -3 to 3
- conv_mixer: float32 [4, 256], replicated, may hold values from -3 to 3
- step_bias: float32 [40], P('chan'), may hold values from -2 to 1
- decay_log: float32 [40], P('chan'), as said below
- skip_gain: float32 [40], P('chan'), may hold values from 0.5 to 1.5
- output_grad: bfloat16 [2, 4096, 2560], P('dp', 'seq', 'chan'), may hold values from -6 to 6
Outputs:
- input_grad: bfloat16 [2, 4096, 2560], P('dp', ('seq', 'chan'))
- inner_weight_grad: float32 [2560, 2560], P(('dp', 'seq'), 'chan')
- mixer_weight_grad: float32 [2560, 256], P(('dp', 'seq', 'chan'))
- step_weight_grad: float32 [2560, 40], P(('dp', 'seq'), 'chan')
The draws below stay inside these ranges and needn't reach their ends.
Inputs may be any that keep to these rules, and one draw needn't show every extreme that they name: exp(decay_log) is at least 0.2 / 4096.
All inputs are finite; a program needn't handle non-finite values.
Results may differ from the reference program's by a relative error of at most 0.014.
Values may be sent and summed in bfloat16 or wider, within the bound.
No kernel may reach another device: no remote copies, remote signals or barrier semaphores. Data moves between devices by JAX's collectives and lax.ppermute only.
A program may use at most 128 MiB of HBM per device.

```python
import math
import jax
import jax.numpy as jnp
from jax import lax

D = 2560
HEADS = 40
HDIM = 64
STATE = 128
KW = 4
BATCH = 2
LENGTH = 4096
TOKENS = 8192
INNER = 2560


def draw_decay_log(key, part):
    base = jax.random.fold_in(key, 71)
    order_key, slow_key, fast_key = jax.random.split(base, 3)
    ranks = jax.random.permutation(order_key, HEADS)
    slow_count = HEADS // 2
    is_slow = ranks < slow_count
    slow_rate = jnp.exp(jax.random.uniform(slow_key, (HEADS,), jnp.float32, jnp.log(0.2), jnp.log(2.0))) / LENGTH
    fast_rate = jnp.exp(jax.random.uniform(fast_key, (HEADS,), jnp.float32, jnp.log(0.02), jnp.log(0.06)))
    return jnp.log(jnp.where(is_slow, slow_rate, fast_rate)).astype(jnp.float32)


def spiked(entries, own_key, source, target, parts, factor):
    def block_of(dim):
        return (jnp.arange(entries.shape[dim]) // (entries.shape[dim] // parts)).reshape((-1,) + (1,) * (entries.ndim - 1 - dim))

    first = jax.random.permutation(own_key, parts)[block_of(target)]
    other_side = (block_of(target) + parts // 2) % parts
    return jnp.where((block_of(source) == first) | (block_of(source) == other_side), factor * entries, entries)


def shard_levels(key, dims, cuts, least, top_value):
    gain = 1.0
    for position, shards_of in cuts:
        steps = jax.random.uniform(jax.random.fold_in(jax.random.fold_in(key, 6), position), (shards_of,), jnp.float32, least / len(cuts), top_value / len(cuts))
        gain = gain * jnp.repeat(jnp.exp(steps), dims[position] // shards_of).reshape((-1,) + (1,) * (len(dims) - 1 - position))
    return gain


def gaussian(stream_key, shape, width, most, cuts=(), held_as=jnp.bfloat16):
    values = jax.random.normal(stream_key, shape, jnp.float32) * width
    if len(cuts) > 0:
        values = shard_levels(stream_key, shape, cuts, -0.22, 0.18) * values
    return jnp.clip(values, min=-most, max=most).astype(held_as)


def noise_with(own_key, dims, width, most, cuts, heavy, kind=jnp.bfloat16):
    drawn = width * jax.random.normal(own_key, dims, jnp.float32)
    if cuts:
        drawn = drawn * shard_levels(own_key, dims, cuts, -0.22, 0.18)
    return jnp.clip(spiked(drawn, jax.random.fold_in(own_key, 3), *heavy), -most, most).astype(kind)


def setup_inputs(seed: int = 0) -> dict:
    splits = jax.random.split(jax.random.key(seed), 11)
    return {
        "layer_input": noise_with(splits[0], (BATCH, LENGTH, D), 1.0, 24.0, ((0, 2), (1, 128)), (1, 2, 128, 5.5)),
        "inner_weight": gaussian(splits[1], (D, INNER), D ** -0.5, 0.125, ((1, 4),)),
        "mixer_weight": gaussian(splits[2], (D, 2 * STATE), (0.1 / D ** 0.5), 0.01171875),
        "step_weight": gaussian(splits[3], (D, HEADS), D ** -0.5, 0.125, ((1, 4),)),
        "conv_inner": gaussian(splits[4], (KW, INNER), KW ** -0.5, 3.0, ((1, 4),), jnp.float32),
        "conv_mixer": gaussian(splits[5], (KW, 2 * STATE), KW ** -0.5, 3.0, (), jnp.float32),
        "step_bias": jnp.clip(-2.0 + 3.0 * jax.random.uniform(splits[6], (HEADS,), jnp.float32) ** shard_levels(splits[6], (HEADS,), ((0, 4),), -0.2, 0.2), -2.0, 1.0),
        "decay_log": draw_decay_log(jax.random.fold_in(splits[10], 71), 0),
        "skip_gain": jnp.clip(0.5 + 1.0 * jax.random.uniform(splits[8], (HEADS,), jnp.float32) ** shard_levels(splits[8], (HEADS,), ((0, 4),), -0.2, 0.2), 0.5, 1.5),
        "output_grad": gaussian(splits[9], (BATCH, LENGTH, INNER), 1.0, 6.0, ((0, 2), (1, 32), (2, 4))),
    }


block_tokens = 256

def conv_silu(inputs, history, kernel):
    length = inputs.shape[0]
    padded = jnp.concatenate([history, inputs], axis=0)
    summed = kernel[0][None, :] * padded[0:length]
    for offset in range(1, kernel.shape[0]):
        summed = summed + kernel[offset][None, :] * padded[offset:offset + length]
    return jax.nn.silu(summed)

def activations(inner_proj, mixer_proj, step_raw, inner_hist, mixer_hist, conv_inner, conv_mixer, step_bias, decay_log):
    length = inner_proj.shape[0]
    head_count = step_bias.shape[0]
    state_width = mixer_proj.shape[1] // 2
    inner_act = conv_silu(inner_proj, inner_hist, conv_inner).reshape(length, head_count, -1)
    mixer_act = conv_silu(mixer_proj, mixer_hist, conv_mixer)
    step_size = jax.nn.softplus(step_raw + step_bias[None, :])
    log_decay = -step_size * jnp.exp(decay_log)[None, :]
    return (inner_act, mixer_act[:, :state_width], mixer_act[:, state_width:], step_size, log_decay)

def spanned_scan(inner_act, input_mix, output_mix, step_size, log_decay, skip_gain, initial):
    length, head_count, head_dim = inner_act.shape
    block_len = min(block_tokens, length)
    blocks = length // block_len
    highest = lax.Precision.HIGHEST

    def to_blocks(values):
        return values.reshape((blocks, block_len) + values.shape[1:])

    def advance(carry_state, pieces):
        part_inner, part_input, part_output, part_step, part_decay = pieces
        cumulative = jnp.cumsum(part_decay, axis=0)
        scores = jnp.dot(part_output, part_input.T, precision=highest)
        causal = (jnp.arange(block_len)[:, None] >= jnp.arange(block_len)[None, :])[:, :, None]
        spread = cumulative[:, None, :] - cumulative[None, :, :]
        weights = jnp.where(causal, jnp.exp(jnp.where(causal, spread, 0.0)), 0.0)
        weights = weights * scores[:, :, None] * part_step[None, :, :]
        within = jnp.einsum('ijh,jhp->ihp', weights, part_inner, precision=highest)
        carried = jnp.exp(cumulative)[:, :, None] * jnp.einsum('in,hpn->ihp', part_output, carry_state, precision=highest)
        result = within + carried + skip_gain[None, :, None] * part_inner
        tail_weight = jnp.exp(cumulative[-1][None, :] - cumulative) * part_step
        update_term = jnp.einsum('jh,jhp,jn->hpn', tail_weight, part_inner, part_input, precision=highest)
        carry_state = jnp.exp(cumulative[-1])[:, None, None] * carry_state + update_term
        return (carry_state, result)
    final, results = lax.scan(jax.checkpoint(advance), initial, (to_blocks(inner_act), to_blocks(input_mix), to_blocks(output_mix), to_blocks(step_size), to_blocks(log_decay)))
    return (results.reshape(length, head_count, head_dim), final)

def contract_rows(left_rows, right_rows):
    return lax.dot_general(left_rows, right_rows, (((0,), (0,)), ((), ())), preferred_element_type=jnp.float32)

def project_back(gradient, weight):
    return lax.dot_general(gradient, weight, (((1,), (1,)), ((), ())), preferred_element_type=jnp.float32)

def reference(layer_input, inner_weight, mixer_weight, step_weight, conv_inner, conv_mixer, step_bias, decay_log, skip_gain, output_grad):
    history_len = KW - 1
    highest = lax.Precision.HIGHEST
    inner_acc = jnp.zeros((D, INNER), jnp.float32)
    mixer_acc = jnp.zeros((D, 2 * STATE), jnp.float32)
    step_acc = jnp.zeros((D, HEADS), jnp.float32)
    input_grads = []
    zero_inner = jnp.zeros((history_len, INNER), jnp.float32)
    zero_mixer = jnp.zeros((history_len, 2 * STATE), jnp.float32)
    initial = jnp.zeros((HEADS, HDIM, STATE), jnp.float32)
    for batch_row in range(BATCH):
        tokens = layer_input[batch_row]
        inner_proj = jnp.dot(tokens, inner_weight, preferred_element_type=jnp.float32).astype(jnp.bfloat16)
        mixer_proj = jnp.dot(tokens, mixer_weight, preferred_element_type=jnp.float32).astype(jnp.bfloat16)
        step_raw = jnp.dot(tokens, step_weight, preferred_element_type=jnp.float32)
        inner_wide = lax.optimization_barrier(inner_proj).astype(jnp.float32)
        mixer_wide = lax.optimization_barrier(mixer_proj).astype(jnp.float32)

        def layer(inner_in, mixer_in, step_in):
            acts = activations(inner_in, mixer_in, step_in, zero_inner, zero_mixer, conv_inner, conv_mixer, step_bias, decay_log)
            result, final = spanned_scan(acts[0], acts[1], acts[2], acts[3], acts[4], skip_gain, initial)
            return result.reshape(LENGTH, INNER)
        unused, pull = jax.vjp(layer, inner_wide, mixer_wide, step_raw)
        grad_inner, grad_mixer, grad_step = pull(output_grad[batch_row].astype(jnp.float32))
        grad_inner = grad_inner.astype(jnp.bfloat16)
        grad_step = grad_step.astype(jnp.bfloat16)
        summed = project_back(grad_inner, inner_weight) + project_back(grad_step, step_weight)
        summed = summed + lax.dot_general(grad_mixer, mixer_weight.astype(jnp.float32), (((1,), (1,)), ((), ())), precision=highest)
        input_grads.append(summed.astype(jnp.bfloat16))
        inner_acc = inner_acc + contract_rows(tokens, grad_inner)
        step_acc = step_acc + contract_rows(tokens, grad_step)
        mixer_acc = mixer_acc + lax.dot_general(tokens.astype(jnp.float32), grad_mixer, (((0,), (0,)), ((), ())), precision=highest)
    norm_factor = 1.0 / math.sqrt(TOKENS)
    return (jnp.stack(input_grads, axis=0), inner_acc * norm_factor, mixer_acc * norm_factor, step_acc * norm_factor)
```

```python
import math

import jax
import jax.numpy as jnp
from jax import lax
from jax.experimental import pallas as pl
from jax.experimental.pallas import tpu as pltpu
from jax.sharding import Mesh
from jax.sharding import PartitionSpec as P

HDIM = 64
SEQ = ("seq_0", "seq_1", "seq_2")
PAIRS = ("seq_0", "seq_1")
ROW4 = ("dp", "seq_1")
ROW8 = ("dp", "seq_1", "seq_2")
DP_SEQ = ("dp", "seq_0", "seq_1", "seq_2")
SEQ_CHAN = ("seq_0", "seq_1", "seq_2", "chan")
DP_SEQ_CHAN = ("dp", "seq_0", "seq_1", "seq_2", "chan")

F32 = jnp.float32
BF16 = jnp.bfloat16
HIGHEST = lax.Precision.HIGHEST
HALO = 16


def dot(a, b, ca=1, cb=0, precision=None):
    return lax.dot_general(
        a, b, (((ca,), (cb,)), ((), ())), precision=precision, preferred_element_type=F32
    )


def vmem(count):
    return [pl.BlockSpec(memory_space=pltpu.VMEM) for _ in range(count)]


def smem():
    return pl.BlockSpec(memory_space=pltpu.SMEM)


def call(kernel, outs, ins, scratch=(), flops=0, name=None):
    specs = [
        smem() if (a.dtype == jnp.int32) else pl.BlockSpec(memory_space=pltpu.VMEM) for a in ins
    ]
    return pl.pallas_call(
        kernel,
        out_shape=[jax.ShapeDtypeStruct(s, d) for s, d in outs],
        in_specs=specs,
        out_specs=vmem(len(outs)),
        scratch_shapes=list(scratch),
        compiler_params=pltpu.CompilerParams(vmem_limit_bytes=48 << 20),
        cost_estimate=pl.CostEstimate(flops=flops, transcendentals=0, bytes_accessed=1 << 20),
        name=name,
    )(*ins)


def heads_to_lanes(heads, width):
    head = lax.broadcasted_iota(jnp.int32, (heads, width), 0)
    lane = lax.broadcasted_iota(jnp.int32, (heads, width), 1)
    return (lane // HDIM == head).astype(F32)


def lanes_to_heads(width, heads):
    lane = lax.broadcasted_iota(jnp.int32, (width, heads), 0)
    head = lax.broadcasted_iota(jnp.int32, (width, heads), 1)
    return (lane // HDIM == head).astype(F32)


def lower(size):
    row = lax.broadcasted_iota(jnp.int32, (size, size), 0)
    col = lax.broadcasted_iota(jnp.int32, (size, size), 1)
    return row >= col


def silu_and_slope(v):
    gate = 1.0 / (1.0 + jnp.exp(-v))
    return v * gate, gate * (1.0 + v * (1.0 - gate))


def project_kernel(
    who, x0, x1, x2, x3, h0, h1, h2, h3, w_in, w_mix, w_step, k_in, k_mix, bias, decay_log, g,
    x_out, act, slope, mix, mix_slope, small, gate_out, rows, zs_out, zg_out, keep, send,
    xs, pi, pm,
):
    chan, core = who[0], who[1]
    part = x0.shape[0]
    tokens = 4 * part
    width = act.shape[1]
    heads = bias.shape[1]
    for k, x in enumerate((x0, x1, x2, x3)):
        slot = lax.rem(chan + 4 - k, 4)
        xs[pl.ds(pl.multiple_of(HALO + slot * part, 16), part), :] = x[...]
    xs[0:HALO, :] = h0[...] + h1[...] + h2[...] + h3[...]
    everything = xs[...]
    x_out[...] = xs[HALO:, :]
    pi[...] = dot(everything, w_in[...]).astype(BF16).astype(F32)
    pm[...] = dot(everything, w_mix[...]).astype(BF16).astype(F32)
    raw = dot(xs[HALO:, :], w_step[...]) + bias[...]

    def convolved(source, kernel):
        total = kernel[3:4, :] * source[HALO:, :]
        for k in range(3):
            start = HALO - 3 + k
            total = total + kernel[k : k + 1, :] * source[start : start + tokens, :]
        return total

    inner_act, inner_slope = silu_and_slope(convolved(pi, k_in))
    act[...] = inner_act
    slope[...] = inner_slope
    mix_act, mixer_slope = silu_and_slope(convolved(pm, k_mix))
    mix[...] = mix_act
    mix_slope[...] = mixer_slope

    step = jnp.maximum(raw, 0.0) + jnp.log1p(jnp.exp(-jnp.abs(raw)))
    gate_out[...] = 1.0 / (1.0 + jnp.exp(-raw))
    decay = -step * jnp.exp(decay_log[...])
    low = lower(tokens).astype(F32)
    total = dot(low, decay, precision=HIGHEST)
    rows[0] = dot(decay, low, 0, 1, precision=HIGHEST)
    row = lax.broadcasted_iota(jnp.int32, (tokens, tokens), 0)
    col = lax.broadcasted_iota(jnp.int32, (tokens, tokens), 1)
    rows[1] = dot(step, (row == col).astype(F32), 0, 0, precision=HIGHEST)
    last = total[tokens - 1 : tokens, :]
    ea = jnp.exp(total)
    tail = jnp.exp(last - total)
    small[0] = step
    small[1] = total
    small[2] = ea
    small[3] = tail
    spread = heads_to_lanes(heads, width)
    wide = dot(jnp.concatenate([tail * step, ea], axis=0), spread, precision=HIGHEST)
    zs = (wide[:tokens] * inner_act).astype(BF16)
    zg = (wide[tokens:] * g[...].astype(F32)).astype(BF16)
    zs_out[...] = zs
    zg_out[...] = zg
    state_width = mix_act.shape[1] // 2
    into = mix_act[:, :state_width].astype(BF16)
    out_of = mix_act[:, state_width:].astype(BF16)
    state = dot(into, zs, 0, 0)
    grad = dot(out_of, zg, 0, 0)
    lead = last.astype(BF16).astype(F32)
    rest = (last - lead).astype(BF16).astype(F32)
    pad = jnp.zeros((14, heads), F32)
    marks = dot(jnp.concatenate([lead, rest, pad], axis=0), spread, precision=HIGHEST).astype(BF16)
    keep[state_width:, :] = marks.astype(F32)
    send[state_width:, :] = marks

    @pl.when(core == 0)
    def _():
        keep[:state_width, :] = state
        send[:state_width, :] = grad.astype(BF16)

    @pl.when(core != 0)
    def _():
        keep[:state_width, :] = grad
        send[:state_width, :] = state.astype(BF16)


def pair_kernel(keep, recv, out):
    n = keep.shape[0] - 16
    width = keep.shape[1]
    own = keep[n : n + 1, :] + keep[n + 1 : n + 2, :]
    other = recv[n:, :].astype(F32)
    theirs = other[0:1, :] + other[1:2, :]
    pair = jnp.exp(theirs) * keep[:n, :] + recv[:n, :].astype(F32)
    total = own + theirs
    lead = total.astype(BF16)
    rest = (total - lead.astype(F32)).astype(BF16)
    groups = out.shape[0]
    per = n // groups
    for k in range(groups):
        out[k, :per, :] = pair[k * per : (k + 1) * per, :].astype(BF16)
        out[k, per : per + 1, :] = lead
        out[k, per + 1 : per + 2, :] = rest


def chain_kernel(who, recv, out):
    forward = who[1] == 0
    groups = recv.shape[0]
    per = out.shape[1]

    def step(k, state):
        slot = jnp.where(forward, k, groups - 1 - k)
        piece = recv[slot].astype(F32)
        out[slot] = state.astype(BF16)
        factor = jnp.exp(piece[per : per + 1, :] + piece[per + 1 : per + 2, :])
        return factor * state + piece[:per, :]

    lax.fori_loop(0, groups, step, jnp.zeros(out.shape[1:], F32), unroll=True)


def back_kernel(keep, before, own, send):
    n = keep.shape[0] - 16
    factor = jnp.exp(keep[n : n + 1, :] + keep[n + 1 : n + 2, :])
    groups, per = before.shape[0], before.shape[1]
    for k in range(groups):
        piece = before[k].astype(F32)
        rows = slice(k * per, (k + 1) * per)
        own[rows, :] = before[k]
        send[rows, :] = (factor * piece + keep[rows, :]).astype(BF16)


def within_kernel(act, mix, g, small, rows, u_out, row_out, col_out, mix_out):
    tokens, width = act.shape
    heads = small.shape[2]
    state_width = mix.shape[1] // 2
    into = mix[:, :state_width].astype(BF16)
    out_of = mix[:, state_width:].astype(BF16)
    scores = dot(out_of, into, 1, 1)
    causal = lower(tokens)
    lane = lax.broadcasted_iota(jnp.int32, (tokens, 128), 1)
    pull = jnp.zeros((tokens, tokens), F32)
    for pair in range(width // 128):
        lanes = slice(pair * 128, (pair + 1) * 128)
        x_pair = act[:, lanes].astype(BF16)
        g_pair = g[:, lanes]
        u_pair = jnp.zeros((tokens, 128), F32)
        for half in range(2):
            h = 2 * pair + half
            g_head = jnp.where(lane // HDIM == half, g_pair, jnp.zeros_like(g_pair))
            inner = dot(g_head, x_pair, 1, 1)
            spread = small[1, :, h : h + 1] - rows[0, h : h + 1, :]
            decay = jnp.where(causal, jnp.exp(jnp.where(causal, spread, 0.0)), 0.0)
            weights = decay * scores
            u_pair = u_pair + dot(weights.astype(BF16), g_head, 0, 0)
            step_row = rows[1, h : h + 1, :]
            both = weights * inner
            col_out[h : h + 1, :] = jnp.sum(both, axis=0, keepdims=True)
            row_out[:, h : h + 1] = jnp.sum(both * step_row, axis=1, keepdims=True)
            pull = pull + decay * inner * step_row
        u_out[:, lanes] = u_pair
    pull = pull.astype(BF16)
    mix_out[:, :state_width] = dot(pull, out_of, 0, 0)
    mix_out[:, state_width:] = dot(pull, into)


def back_through_kernel(
    who, own, other, act, slope, mix, mix_slope, g, small, gate, zs, zg, u, row_in, col_in, mix_in,
    decay_log, skip, pre_out, head_out, step_out, s0, gt,
):
    tokens, width = act.shape
    heads = small.shape[2]
    state_width = mix.shape[1] // 2

    @pl.when(who[1] == 0)
    def _():
        s0[...] = own[...]
        gt[...] = other[...]

    @pl.when(who[1] != 0)
    def _():
        s0[...] = other[...]
        gt[...] = own[...]

    into = mix[:, :state_width].astype(BF16)
    out_of = mix[:, state_width:].astype(BF16)
    gb = dot(into, gt[...])
    sc = dot(out_of, s0[...])
    step = small[0]
    spread = heads_to_lanes(heads, width)
    gather = lanes_to_heads(width, heads)
    skip_rows = jnp.broadcast_to(skip[...], (8, heads))
    wide = dot(
        jnp.concatenate([step, small[3], skip_rows], axis=0), spread, precision=HIGHEST
    )
    tail_gb = wide[tokens : 2 * tokens] * gb
    x = act[...]
    upstream = g[...].astype(F32)
    d_act = wide[:tokens] * (u[...] + tail_gb) + wide[2 * tokens : 2 * tokens + 1] * upstream
    d_pre = d_act * slope[...]
    pre_out[:, :width] = d_pre
    cross = jnp.sum(gt[...].astype(F32) * s0[...].astype(F32), axis=0, keepdims=True)
    sums = dot(
        jnp.concatenate(
            [x * tail_gb, zg[...].astype(F32) * sc, jnp.broadcast_to(cross, (8, width))], axis=0
        ),
        gather,
        precision=HIGHEST,
    )
    e_part = sums[:tokens]
    c_part = sums[tokens : 2 * tokens]
    f_part = sums[2 * tokens : 2 * tokens + 1]
    row = lax.broadcasted_iota(jnp.int32, (tokens, tokens), 0)
    col = lax.broadcasted_iota(jnp.int32, (tokens, tokens), 1)
    col_part = dot((row == col).astype(F32), col_in[...], 1, 1, precision=HIGHEST)
    e_step = step * e_part
    d_total = row_in[...] + c_part - step * col_part - e_step
    at_end = jnp.sum(e_step, axis=0, keepdims=True) + small[2, tokens - 1 : tokens, :] * f_part
    d_decay = dot((row <= col).astype(F32), d_total, precision=HIGHEST) + at_end
    d_step = col_part + e_part - d_decay * jnp.exp(decay_log[...])
    step_out[...] = jnp.zeros_like(step_out)
    step_out[:, :heads] = (d_step * gate[...]).astype(BF16)
    d_into = mix_in[:, :state_width] + dot(zs[...], gt[...], 1, 1)
    d_out_of = mix_in[:, state_width:] + dot(zg[...], s0[...], 1, 1)
    pre_out[:, width : width + state_width] = d_into * mix_slope[:, :state_width]
    pre_out[:, width + state_width :] = d_out_of * mix_slope[:, state_width:]
    head_out[...] = pre_out[0:8, :]


def conv_back_kernel(pre, ahead, step, k_in, k_mix, out, padded):
    tokens = pre.shape[0]
    width = k_in.shape[1]
    padded[:tokens, :] = pre[...]
    padded[tokens:, :] = ahead[...]

    def convolved(lanes, kernel):
        total = kernel[3:4, :] * padded[:tokens, lanes]
        for k in range(3):
            total = total + kernel[k : k + 1, :] * padded[3 - k : 3 - k + tokens, lanes]
        return total

    edge = pre.shape[1]
    out[:, :width] = convolved(slice(0, width), k_in).astype(BF16)
    out[:, width:edge] = convolved(slice(width, edge), k_mix).astype(BF16)
    out[:, edge:] = step[...]


def input_grad_kernel(grads, w_in, w_mix, w_step, out):
    width = w_in.shape[1]
    edge = width + w_mix.shape[1]
    heads = w_step.shape[1]
    total = dot(grads[:, :width], w_in[...], 1, 1)
    total = total + dot(grads[:, width:edge], w_mix[...], 1, 1)
    total = total + dot(grads[:, edge : edge + heads], w_step[...], 1, 1)
    out[...] = total.astype(BF16).reshape(out.shape)


def weight_grad_kernel(who, xt, g0, g1, g2, g3, s0, s1, s2, s3, inner_out, mix_out):
    core, place = who[1], who[2]
    total = None
    for k, (same, swapped) in enumerate(((g0, s0), (g1, s1), (g2, s2), (g3, s3))):
        source = 2 * lax.rem(place + 4 - k, 4)
        total_k = dot(xt[source + core], same[...]) + dot(xt[source + 1 - core], swapped[...])
        total = total_k if total is None else total + total_k
    width = 640
    rows = inner_out.shape[1]
    for k in range(inner_out.shape[0]):
        part = slice(k * rows, (k + 1) * rows)
        inner_out[k, :, :width] = total[part, :width].astype(BF16)
        inner_out[k, :, width:] = total[part, width + 256 :].astype(BF16)
    mix_out[...] = total[:, width : width + 256].astype(BF16)


def a2a(value, axis):
    return lax.all_to_all(value, axis, split_axis=0, concat_axis=0, tiled=True)


def turned(value, axis, steps):
    count = lax.axis_size(axis)
    return lax.ppermute(value, axis, [(k, (k + steps) % count) for k in range(count)])


def body(
    layer_input,
    inner_weight,
    mixer_weight,
    step_weight,
    conv_inner,
    conv_mixer,
    step_bias,
    decay_log,
    skip_gain,
    output_grad,
):
    own = layer_input[0]
    part, model = own.shape
    chans = lax.axis_size("chan")
    tokens = part * chans
    width = inner_weight.shape[1]
    heads = step_bias.shape[0]
    mixed = mixer_weight.shape[1]
    state_width = mixed // 2
    g = output_grad[0]
    who = jnp.stack(
        [lax.axis_index("chan"), lax.axis_index("seq_2"), lax.axis_index(ROW4)]
    ).astype(jnp.int32)
    bias = step_bias[None]
    rate = decay_log[None]
    skip = skip_gain[None]

    arrived = [own] + [turned(own, "chan", k) for k in (1, 2, 3)]
    tail_rows = own[part - HALO :]
    seq_count = lax.axis_size(SEQ)
    halos = [
        lax.ppermute(
            tail_rows,
            SEQ_CHAN,
            [(s * chans + chans - 1, (s + 1) * chans + c) for s in range(seq_count - 1)],
        )
        for c in range(chans)
    ]
    t, c = tokens, width
    x, act, slope, mix, mix_slope, small, gate, rows, zs, zg, keep, send = call(
        project_kernel,
        [
            ((t, model), BF16),
            ((t, c), F32),
            ((t, c), F32),
            ((t, mixed), F32),
            ((t, mixed), F32),
            ((4, t, heads), F32),
            ((t, heads), F32),
            ((2, heads, t), F32),
            ((t, c), BF16),
            ((t, c), BF16),
            ((state_width + 16, c), F32),
            ((state_width + 16, c), BF16),
        ],
        [
            who, *arrived, *halos, inner_weight, mixer_weight, step_weight, conv_inner,
            conv_mixer, bias, rate, g,
        ],
        [
            pltpu.VMEM((t + HALO, model), BF16),
            pltpu.VMEM((t + HALO, c), F32),
            pltpu.VMEM((t + HALO, mixed), F32),
        ],
        flops=700_000_000,
        name="project",
    )
    got = turned(send, "seq_2", 1)
    groups = lax.axis_size(PAIRS)
    per = state_width // groups
    (pairs,) = call(pair_kernel, [((groups, 2 * per, c), BF16)], [keep, got], name="pair")
    pairs = a2a(pairs, PAIRS)

    u, row_part, col_part, mix_part = call(
        within_kernel,
        [((t, c), F32), ((t, heads), F32), ((heads, t), F32), ((t, mixed), F32)],
        [act, mix, g, small, rows],
        flops=700_000_000,
        name="within",
    )
    group8 = lax.axis_size(ROW8)
    share = model // (lax.axis_size(DP_SEQ))
    lines = lax.axis_size("seq_0")
    xt = x.T.reshape(lax.axis_size("dp"), lines, group8 // 2, share, t)
    xt = jnp.swapaxes(xt, 1, 2).reshape(group8, lines * share, t)
    xt = a2a(xt, ROW8)

    (befores,) = call(chain_kernel, [((groups, per, c), BF16)], [who, pairs], name="chain")
    befores = a2a(befores, PAIRS)
    mine, others = call(
        back_kernel, [((state_width, c), BF16)] * 2, [keep, befores], name="back"
    )
    others = turned(others, "seq_2", 1)
    pre, head, step_grad = call(
        back_through_kernel,
        [((t, c + mixed), F32), ((8, c + mixed), F32), ((t, 128), BF16)],
        [
            who, mine, others, act, slope, mix, mix_slope, g, small, gate, zs, zg, u, row_part,
            col_part, mix_part, rate, skip,
        ],
        [pltpu.VMEM((state_width, c), BF16), pltpu.VMEM((state_width, c), BF16)],
        flops=500_000_000,
        name="through",
    )
    ahead = lax.ppermute(head, SEQ, [(k + 1, k) for k in range(seq_count - 1)])
    (grads,) = call(
        conv_back_kernel,
        [((t, c + mixed + 128), BF16)],
        [pre, ahead, step_grad, conv_inner, conv_mixer],
        [pltpu.VMEM((t + 8, c + mixed), F32)],
        name="conv_back",
    )
    same = [grads] + [turned(grads, ROW4, k) for k in (1, 2, 3)]
    swapped = [turned(v, "seq_2", 1) for v in same]
    (partial,) = call(
        input_grad_kernel,
        [((chans, part, model), BF16)],
        [grads, inner_weight, mixer_weight, step_weight],
        flops=500_000_000,
        name="input_grad",
    )
    input_grad = a2a(partial, "chan").astype(F32).sum(axis=0).astype(BF16)
    inner_terms, mixer_terms = call(
        weight_grad_kernel,
        [((lines, share, c + 128), BF16), ((lines * share, mixed), BF16)],
        [who, xt, *same, *swapped],
        flops=700_000_000,
        name="weight_grad",
    )
    norm = 1.0 / math.sqrt(tokens * seq_count * lax.axis_size("dp"))
    mixer_terms = a2a(mixer_terms.reshape(lines * chans, share // chans, mixed), ("seq_0", "chan"))
    inner_terms = a2a(inner_terms, "seq_0")
    summed = inner_terms.astype(F32).sum(axis=0) * norm
    mixer_weight_grad = mixer_terms.astype(F32).sum(axis=0) * norm
    return (
        input_grad[None],
        summed[:, :c],
        mixer_weight_grad,
        summed[:, c : c + heads],
    )


def solution(mesh):
    split = Mesh(
        mesh.devices.reshape(mesh.shape["dp"], 8, 2, 2, mesh.shape["chan"]),
        ("dp", "seq_0", "seq_1", "seq_2", "chan"),
    )
    placed = (
        P("dp", SEQ_CHAN, None),
        P(None, "chan"),
        P(),
        P(None, "chan"),
        P(None, "chan"),
        P(),
        P("chan"),
        P("chan"),
        P("chan"),
        P("dp", SEQ, "chan"),
    )
    return jax.shard_map(
        body,
        mesh=split,
        in_specs=placed,
        out_specs=(
            P("dp", SEQ_CHAN, None),
            P(DP_SEQ, "chan"),
            P(DP_SEQ_CHAN, None),
            P(DP_SEQ, "chan"),
        ),
        check_vma=False,
    )
```

```python
import math

import jax
import jax.numpy as jnp
from jax import lax
from jax.experimental import pallas as pl
from jax.experimental.pallas import tpu as pltpu
from jax.sharding import Mesh
from jax.sharding import PartitionSpec as P


HDIM = 64
SEQ = ("seq_0", "seq_1", "seq_2")
PAIRS = ("seq_0", "seq_1")
ROW4 = ("dp", "seq_1")
ROW8 = ("dp", "seq_1", "seq_2")
DP_SEQ = ("dp", "seq_0", "seq_1", "seq_2")
SEQ_CHAN = ("seq_0", "seq_1", "seq_2", "chan")
DP_SEQ_CHAN = ("dp", "seq_0", "seq_1", "seq_2", "chan")

F32 = jnp.float32
BF16 = jnp.bfloat16
HIGHEST = lax.Precision.HIGHEST
HALO = 16


def dot(a, b, ca=1, cb=0, precision=None):
    return lax.dot_general(
        a, b, (((ca,), (cb,)), ((), ())), precision=precision, preferred_element_type=F32
    )


def in_hbm(value):
    return pltpu.with_memory_space_constraint(value, pltpu.HBM)


def call(kernel, outs, ins, loads=(), stores=(), scratch=(), flops=0, early=False):
    count = len(ins)

    def wrapped(*refs):
        refs = list(refs)
        operands, results = refs[:count], refs[count : count + len(outs)]
        spare = refs[count + len(outs) :]
        sems = spare.pop()
        copies = []
        for k, position in enumerate(loads):
            buffer = spare.pop(0)
            copies.append(pltpu.make_async_copy(operands[position], buffer, sems.at[k]))
            operands[position] = buffer
        for copy in copies:
            copy.start()
        pending = {}
        for k, position in enumerate(stores):
            buffer = spare.pop(0)
            pending[position] = pltpu.make_async_copy(
                buffer, results[position], sems.at[len(loads) + k]
            )
            results[position] = buffer
        for copy in copies:
            copy.wait()
        started = []

        def flush(position):
            pending[position].start()
            started.append(position)

        if early:
            kernel(*operands, *results, *spare, flush=flush)
        else:
            kernel(*operands, *results, *spare)
        for position in stores:
            if position not in started:
                pending[position].start()
        for position in stores:
            pending[position].wait()

    specs, values = [], []
    for k, a in enumerate(ins):
        space = pltpu.VMEM
        if a.dtype == jnp.int32:
            space = pltpu.SMEM
        elif k in loads:
            space = pltpu.HBM
            a = in_hbm(a)
        specs.append(pl.BlockSpec(memory_space=space))
        values.append(a)
    buffers = [pltpu.VMEM(ins[k].shape, ins[k].dtype) for k in loads]
    buffers += [pltpu.VMEM(*outs[k]) for k in stores]
    return pl.pallas_call(
            wrapped,
            out_shape=[
                pltpu.HBM(s, d) if k in stores else jax.ShapeDtypeStruct(s, d)
                for k, (s, d) in enumerate(outs)
            ],
            in_specs=specs,
            out_specs=[
                pl.BlockSpec(memory_space=pltpu.HBM if k in stores else pltpu.VMEM)
                for k in range(len(outs))
            ],
            scratch_shapes=buffers
            + list(scratch)
            + [pltpu.SemaphoreType.DMA((len(loads) + len(stores) + 1,))],
            compiler_params=pltpu.CompilerParams(vmem_limit_bytes=24 << 20),
            cost_estimate=pl.CostEstimate(flops=flops, transcendentals=0, bytes_accessed=1 << 20),
    )(*values)


def heads_to_lanes(heads, width):
    head = lax.broadcasted_iota(jnp.int32, (heads, width), 0)
    lane = lax.broadcasted_iota(jnp.int32, (heads, width), 1)
    return (lane // HDIM == head).astype(F32)


def lanes_to_heads(width, heads):
    lane = lax.broadcasted_iota(jnp.int32, (width, heads), 0)
    head = lax.broadcasted_iota(jnp.int32, (width, heads), 1)
    return (lane // HDIM == head).astype(F32)


def lower(size):
    row = lax.broadcasted_iota(jnp.int32, (size, size), 0)
    col = lax.broadcasted_iota(jnp.int32, (size, size), 1)
    return row >= col


def silu_and_slope(v):
    gate = 1.0 / (1.0 + jnp.exp(-v))
    return v * gate, gate * (1.0 + v * (1.0 - gate))


def load_kernel(*refs):
    half = len(refs) // 2
    for source, out in zip(refs[:half], refs[half:]):
        out[...] = source[...]


def project_kernel(
    who, x0, x1, x2, x3, h0, h1, h2, h3, w_in, w_mix, w_step, k_in, k_mix, bias, decay_log, g,
    x_out, big, z_out, small, rows, keep, send, kept,
    xs, pi, pm, *, flush,
):
    chan, core = who[0], who[1]
    part = x0.shape[0]
    tokens = 4 * part
    width = k_in.shape[1]
    mixed = k_mix.shape[1]
    state_width = mixed // 2
    heads = bias.shape[1]
    for k, x in enumerate((x0, x1, x2, x3)):
        slot = lax.rem(chan + 4 - k, 4)
        xs[pl.ds(pl.multiple_of(HALO + slot * part, 16), part), :] = x[...]
    edge = h0.shape[0]
    xs[0:HALO, :] = jnp.zeros_like(xs[0:HALO, :])
    xs[0:edge, :] = h0[...] + h1[...] + h2[...] + h3[...]
    everything = xs[...]
    x_out[...] = xs[HALO:, :]
    flush(0)
    pi[...] = dot(everything, w_in[...]).astype(BF16).astype(F32)
    pm[...] = dot(everything, w_mix[...]).astype(BF16).astype(F32)
    pi[HALO - edge : HALO, :] = pi[0:edge, :]
    pm[HALO - edge : HALO, :] = pm[0:edge, :]
    raw = dot(xs[HALO:, :], w_step[...], 1, 1) + bias[...]

    def convolved(source, kernel):
        total = kernel[3:4, :] * source[HALO:, :]
        for k in range(3):
            start = HALO - 3 + k
            total = total + kernel[k : k + 1, :] * source[start : start + tokens, :]
        return total

    inner_act, inner_slope = silu_and_slope(convolved(pi, k_in))
    big[:, :width] = inner_act
    big[:, width : 2 * width] = inner_slope
    mix_act, mixer_slope = silu_and_slope(convolved(pm, k_mix))
    big[:, 2 * width : 2 * width + mixed] = mix_act
    big[:, 2 * width + mixed :] = mixer_slope
    flush(1)

    step = jnp.maximum(raw, 0.0) + jnp.log1p(jnp.exp(-jnp.abs(raw)))
    decay = -step * jnp.exp(decay_log[...])
    low = lower(tokens).astype(F32)
    total = dot(low, decay, precision=HIGHEST)
    rows[0] = dot(decay, low, 0, 1, precision=HIGHEST)
    row = lax.broadcasted_iota(jnp.int32, (tokens, tokens), 0)
    col = lax.broadcasted_iota(jnp.int32, (tokens, tokens), 1)
    rows[1] = dot(step, (row == col).astype(F32), 0, 0, precision=HIGHEST)
    last = total[tokens - 1 : tokens, :]
    ea = jnp.exp(total)
    tail = jnp.exp(last - total)
    small[0] = step
    small[1] = total
    small[2] = ea
    small[3] = tail
    small[4] = 1.0 / (1.0 + jnp.exp(-raw))
    spread = heads_to_lanes(heads, width)
    wide = dot(jnp.concatenate([tail * step, ea], axis=0), spread, precision=HIGHEST)
    zs = (wide[:tokens] * inner_act).astype(BF16)
    zg = (wide[tokens:] * g[...].astype(F32)).astype(BF16)
    z_out[:, :width] = zs
    z_out[:, width:] = zg
    for k in (2, 3, 4):
        flush(k)
    into = mix_act[:, :state_width].astype(BF16)
    out_of = mix_act[:, state_width:].astype(BF16)
    state = dot(into, zs, 0, 0)
    grad = dot(out_of, zg, 0, 0)
    lead = last.astype(BF16)
    keep[:, width:] = jnp.zeros_like(keep[:, width:])
    send[:, width:] = jnp.zeros_like(send[:, width:])
    keep[0:1, width : width + heads] = last
    send[0:1, width : width + heads] = lead
    send[1:2, width : width + heads] = (last - lead.astype(F32)).astype(BF16)

    @pl.when(core == 0)
    def _():
        keep[:, :width] = state
        send[:, :width] = grad.astype(BF16)

    @pl.when(core != 0)
    def _():
        keep[:, :width] = grad
        send[:, :width] = state.astype(BF16)

    kept[...] = keep[...]


def pair_kernel(keep, recv, out):
    groups, per = out.shape[0], out.shape[1]
    heads = out.shape[2] // HDIM - 2
    width = heads * HDIM
    spread = heads_to_lanes(heads, width)
    own = keep[0:8, width : width + heads]
    other = recv[0:16, width : width + heads].astype(F32)
    theirs = other[0:1] + other[1:2]
    wide = dot(jnp.broadcast_to(jnp.exp(theirs), (8, heads)), spread, precision=HIGHEST)
    pair = (wide[0:1] * keep[:, :width] + recv[:, :width].astype(F32)).astype(BF16)
    total = own[0:1] + theirs
    lead = total.astype(BF16)
    rest = (total - lead.astype(F32)).astype(BF16)
    out[:, :, :width] = pair.reshape(groups, per, width)
    out[:, :, width:] = jnp.zeros_like(out[:, :, width:])
    for k in range(groups):
        out[k, 0:1, width : width + heads] = lead
        out[k, 1:2, width : width + heads] = rest


def chain_kernel(who, recv, out, factors):
    forward = who[1] == 0
    groups = recv.shape[0]
    width = out.shape[2]
    heads = width // HDIM
    marks = recv[:, 0, width : width + heads].astype(F32)
    marks = marks + recv[:, 1, width : width + heads].astype(F32)
    factors[...] = dot(jnp.exp(marks), heads_to_lanes(heads, width), precision=HIGHEST)

    def step(k, state):
        slot = jnp.where(forward, k, groups - 1 - k)
        out[slot] = state.astype(BF16)
        return factors[pl.ds(slot, 1), :] * state + recv[slot, :, :width].astype(F32)

    lax.fori_loop(0, groups, step, jnp.zeros(out.shape[1:], F32), unroll=True)


def back_kernel(keep, before, own, send):
    groups, per, width = before.shape
    heads = width // HDIM
    last = jnp.broadcast_to(keep[0:1, width : width + heads], (8, heads))
    factor = dot(jnp.exp(last), heads_to_lanes(heads, width), precision=HIGHEST)[0:1]
    piece = before[...].reshape(groups * per, width)
    own[...] = piece
    send[...] = (factor * piece.astype(F32) + keep[:, :width]).astype(BF16)


def pack_kernel(who, x, *refs, half):
    outs, turned_x = refs[:-1], refs[-1]
    core, place = who[1], who[2]
    model = x.shape[1]
    lines = 8
    share = outs[0].shape[0] // lines
    for k in range(model // 128):
        lanes = slice(k * 128, (k + 1) * 128)
        turned_x[lanes, :] = x[:, lanes].astype(F32).T
    for k, out in enumerate(outs):
        steps, flip = divmod(k, 2)
        where = lax.rem(place + steps, 4)
        side = core if flip == 0 else 1 - core
        outer = where // half
        inner = 2 * (where - outer * half) + side
        for line in range(lines):
            start = share * ((outer * lines + line) * 2 * half + inner)
            out[line * share : (line + 1) * share, :] = turned_x[
                pl.ds(pl.multiple_of(start, 8), share), :
            ].astype(BF16)


def within_kernel(big, g, small, rows, u_out, row_out, col_out):
    tokens, width = g.shape
    mixed = (big.shape[1] - 2 * width) // 2
    state_width = mixed // 2
    into = big[:, 2 * width : 2 * width + state_width].astype(BF16)
    out_of = big[:, 2 * width + state_width : 2 * width + mixed].astype(BF16)
    scores = dot(out_of, into, 1, 1)
    causal = lower(tokens)
    lane = lax.broadcasted_iota(jnp.int32, (tokens, 128), 1)
    pull = jnp.zeros((tokens, tokens), F32)
    for pair in range(width // 128):
        lanes = slice(pair * 128, (pair + 1) * 128)
        x_pair = big[:, lanes].astype(BF16)
        g_pair = g[:, lanes]
        u_pair = jnp.zeros((tokens, 128), F32)
        for half in range(2):
            h = 2 * pair + half
            g_head = jnp.where(lane // HDIM == half, g_pair, jnp.zeros_like(g_pair))
            inner = dot(g_head, x_pair, 1, 1)
            spread = small[1, :, h : h + 1] - rows[0, h : h + 1, :]
            decay = jnp.where(causal, jnp.exp(jnp.where(causal, spread, 0.0)), 0.0)
            weights = decay * scores
            u_pair = u_pair + dot(weights.astype(BF16), g_head, 0, 0)
            step_row = rows[1, h : h + 1, :]
            both = weights * inner
            col_out[h : h + 1, :] = jnp.sum(both, axis=0, keepdims=True)
            row_out[:, h : h + 1] = jnp.sum(both * step_row, axis=1, keepdims=True)
            pull = pull + decay * inner * step_row
        u_out[:, lanes] = u_pair
    pull = pull.astype(BF16)
    u_out[:, width : width + state_width] = dot(pull, out_of, 0, 0)
    u_out[:, width + state_width :] = dot(pull, into)


def back_through_kernel(
    who, own, other, big, z, small, u, row_in, col_in, g, decay_log, skip, k_in, k_mix,
    pre_out, head_out, step_out, k_out, s0, gt,
):
    tokens, width = g.shape
    heads = small.shape[2]
    mixed = (big.shape[1] - 2 * width) // 2
    state_width = mixed // 2

    @pl.when(who[1] == 0)
    def _():
        s0[...] = own[...]
        gt[...] = other[...]

    @pl.when(who[1] != 0)
    def _():
        s0[...] = other[...]
        gt[...] = own[...]

    into = big[:, 2 * width : 2 * width + state_width].astype(BF16)
    out_of = big[:, 2 * width + state_width : 2 * width + mixed].astype(BF16)
    zs = z[:, :width]
    zg = z[:, width:]
    gb = dot(into, gt[...])
    sc = dot(out_of, s0[...])
    step = small[0]
    spread = heads_to_lanes(heads, width)
    gather = lanes_to_heads(width, heads)
    skip_rows = jnp.broadcast_to(skip[...], (8, heads))
    wide = dot(
        jnp.concatenate([step, small[3], skip_rows], axis=0), spread, precision=HIGHEST
    )
    tail_gb = wide[tokens : 2 * tokens] * gb
    x = big[:, :width]
    upstream = g[...].astype(F32)
    d_act = wide[:tokens] * (u[:, :width] + tail_gb) + wide[2 * tokens : 2 * tokens + 1] * upstream
    d_pre = d_act * big[:, width : 2 * width]
    pre_out[:, :width] = d_pre
    cross = jnp.sum(gt[...].astype(F32) * s0[...].astype(F32), axis=0, keepdims=True)
    sums = dot(
        jnp.concatenate(
            [x * tail_gb, zg.astype(F32) * sc, jnp.broadcast_to(cross, (8, width))], axis=0
        ),
        gather,
        precision=HIGHEST,
    )
    e_part = sums[:tokens]
    c_part = sums[tokens : 2 * tokens]
    f_part = sums[2 * tokens : 2 * tokens + 1]
    row = lax.broadcasted_iota(jnp.int32, (tokens, tokens), 0)
    col = lax.broadcasted_iota(jnp.int32, (tokens, tokens), 1)
    col_part = dot((row == col).astype(F32), col_in[...], 1, 1, precision=HIGHEST)
    e_step = step * e_part
    d_total = row_in[...] + c_part - step * col_part - e_step
    at_end = jnp.sum(e_step, axis=0, keepdims=True) + small[2, tokens - 1 : tokens, :] * f_part
    d_decay = dot((row <= col).astype(F32), d_total, precision=HIGHEST) + at_end
    d_step = col_part + e_part - d_decay * jnp.exp(decay_log[...])
    step_out[...] = jnp.zeros_like(step_out)
    step_out[:, :heads] = (d_step * small[4]).astype(BF16)
    d_into = u[:, width : width + state_width] + dot(zs, gt[...], 1, 1)
    d_out_of = u[:, width + state_width :] + dot(zg, s0[...], 1, 1)
    slopes = 2 * width + mixed
    pre_out[:, width : width + state_width] = d_into * big[:, slopes : slopes + state_width]
    pre_out[:, width + state_width :] = d_out_of * big[:, slopes + state_width :]
    head_out[...] = pre_out[0:8, :]
    k_out[:, :width] = k_in[...]
    k_out[:, width:] = k_mix[...]


def conv_back_kernel(pre, ahead, step, kernel, out, mix_out, padded):
    tokens = pre.shape[0]
    width = out.shape[1] - 128
    padded[:tokens, :] = pre[...]
    padded[tokens:, :] = ahead[...]

    def convolved(lanes):
        total = kernel[3:4, lanes] * padded[:tokens, lanes]
        for k in range(3):
            total = total + kernel[k : k + 1, lanes] * padded[3 - k : 3 - k + tokens, lanes]
        return total

    out[:, :width] = convolved(slice(0, width)).astype(BF16)
    out[:, width:] = step[...]
    mix_out[...] = convolved(slice(width, pre.shape[1])).astype(BF16)


def input_grad_kernel(who, grads, mix_grads, w_in, w_mix, w_step, *refs):
    outs, whole = refs[:4], refs[4]
    width = w_in.shape[1]
    heads = w_step.shape[0]
    total = dot(grads[:, :width], w_in[...], 1, 1)
    total = total + dot(mix_grads[...], w_mix[...], 1, 1)
    total = total + dot(grads[:, width : width + heads], w_step[...])
    whole[...] = total.astype(BF16)
    part = outs[0].shape[0]
    for k, out in enumerate(outs):
        slot = lax.rem(who[0] + k, 4)
        out[...] = whole[pl.ds(pl.multiple_of(slot * part, 16), part), :]


def add_kernel(m0, m1, m2, m3, out):
    total = m0[...].astype(F32) + m1[...].astype(F32) + m2[...].astype(F32) + m3[...].astype(F32)
    out[...] = total.astype(BF16)


def gathered_product(slabs, grads):
    total = None
    for slab, grad in zip(slabs, grads):
        part = dot(slab[...], grad[...])
        total = part if total is None else total + part
    return total


def inner_weight_kernel(*refs):
    refs[-1][...] = gathered_product(refs[:8], refs[8:16]).astype(BF16)


def mixer_weight_kernel(who, *refs):
    slabs, grads, inner, out = refs[:8], refs[8:16], refs[16], refs[17]
    chan = who[0]
    lines, share, _ = out.shape
    total = gathered_product(slabs, grads).astype(BF16)
    size = lines * share
    few = share // 4
    to_row = lax.broadcasted_iota(jnp.int32, (size, size), 0)
    from_row = lax.broadcasted_iota(jnp.int32, (size, size), 1)
    within_line = to_row - (to_row // share) * share
    group = within_line // few
    wanted = to_row - within_line + chan * few + (within_line - group * few)
    chosen = None
    for q in range(4):
        pick = ((from_row == wanted) & (group == q)).astype(BF16)
        part = dot(pick, total[:, q * 64 : (q + 1) * 64])
        chosen = part if chosen is None else chosen + part
    edge = inner.shape[1] - 64
    out[:, :, :] = inner[...].reshape(out.shape)
    out[:, :, edge:] = chosen.astype(BF16).reshape(lines, share, 64)


def total_kernel(terms, inner_out, mix_out, step_out, whole, *, norm):
    lines, share, _ = terms.shape
    width = inner_out.shape[1]
    few = share // 4
    total = terms[0].astype(F32)
    for k in range(1, lines):
        total = total + terms[k].astype(F32)
    whole[...] = total * norm
    inner_out[...] = whole[:, :width]
    edge = whole.shape[1] - 64
    for q in range(4):
        mix_out[:, q * 64 : (q + 1) * 64] = whole[q * few : (q + 1) * few, edge:]
    heads = step_out.shape[0]
    row = lax.broadcasted_iota(jnp.int32, (heads, 128), 0)
    col = lax.broadcasted_iota(jnp.int32, (heads, 128), 1)
    step_out[...] = dot(
        (row == col).astype(F32), whole[:, width : width + 128], 1, 1, precision=HIGHEST
    )


def a2a(value, axis):
    return lax.all_to_all(value, axis, split_axis=0, concat_axis=0, tiled=True)


def moves(steps, flip, count):
    return [
        (2 * d + c, 2 * ((d + steps) % (count // 2)) + (c ^ flip))
        for d in range(count // 2)
        for c in range(2)
    ]


def turned(value, axis, steps):
    count = lax.axis_size(axis)
    return lax.ppermute(value, axis, [(k, (k + steps) % count) for k in range(count)])


def layer(
    layer_input,
    inner_weight,
    mixer_weight,
    step_weight,
    conv_inner,
    conv_mixer,
    step_bias,
    decay_log,
    skip_gain,
    output_grad,
):
    own = layer_input[0]
    part, model = own.shape
    chans = lax.axis_size("chan")
    tokens = part * chans
    width = inner_weight.shape[1]
    heads = step_bias.shape[0]
    mixed = mixer_weight.shape[1]
    state_width = mixed // 2
    g = output_grad[0]
    who = jnp.stack(
        [lax.axis_index("chan"), lax.axis_index("seq_2"), lax.axis_index(ROW4)]
    ).astype(jnp.int32)
    bias = step_bias[None]
    rate = decay_log[None]
    skip = skip_gain[None]

    seq_count = lax.axis_size(SEQ)
    t, c = tokens, width

    arrived = [turned(own, "chan", k) for k in (1, 2, 3)]
    tail_rows = own[part - 4 :]
    halos = [
        lax.ppermute(
            tail_rows,
            SEQ_CHAN,
            [(s * chans + chans - 1, (s + 1) * chans + k) for s in range(seq_count - 1)],
        )
        for k in range(chans)
    ]
    sources = [
        own, inner_weight, mixer_weight, step_weight.T, conv_inner, conv_mixer, bias, rate, g
    ]
    near = call(
        load_kernel,
        [(v.shape, v.dtype) for v in sources],
        sources,
        loads=tuple(range(len(sources))),
        flops=700_000_000,
    )
    x, big, z, small, rows, keep, send, kept = call(
        project_kernel,
        [
            ((t, model), BF16),
            ((t, 2 * c + 2 * mixed), F32),
            ((t, 2 * c), BF16),
            ((5, t, heads), F32),
            ((2, heads, t), F32),
            ((state_width, c + 128), F32),
            ((state_width, c + 128), BF16),
            ((state_width, c + 128), F32),
        ],
        [who, near[0], *arrived, *halos, *near[1:]],
        stores=(0, 1, 2, 3, 4, 7),
        scratch=[
            pltpu.VMEM((t + HALO, model), BF16),
            pltpu.VMEM((t + HALO, c), F32),
            pltpu.VMEM((t + HALO, mixed), F32),
        ],
        flops=700_000_000,
        early=True,
    )
    got = turned(send, "seq_2", 1)
    groups = lax.axis_size(PAIRS)
    per = state_width // groups
    (pairs,) = call(pair_kernel, [((groups, per, c + 128), BF16)], [keep, got])
    pairs = a2a(pairs, PAIRS)

    u, row_part, col_part = call(
        within_kernel,
        [((t, c + mixed), F32), ((t, heads), F32), ((heads, t), F32)],
        [big, g, small, rows],
        loads=(0, 1, 2, 3),
        stores=(0, 1, 2),
        flops=700_000_000,
    )
    group8 = lax.axis_size(ROW8)
    share = model // lax.axis_size(DP_SEQ)
    lines = lax.axis_size("seq_0")
    slabs = call(
        lambda *refs: pack_kernel(*refs, half=lax.axis_size("seq_1")),
        [((lines * share, t), BF16)] * group8,
        [who, x],
        loads=(1,),
        scratch=[pltpu.VMEM((model, t), F32)],
        flops=500_000_000,
    )
    slabs = [slabs[0]] + [
        lax.ppermute(slabs[k], ROW8, moves(k // 2, k % 2, group8)) for k in range(1, group8)
    ]

    (befores,) = call(
        chain_kernel,
        [((groups, per, c), BF16)],
        [who, pairs],
        scratch=[pltpu.VMEM((groups, c), F32)],
    )
    befores = a2a(befores, PAIRS)
    mine, others = call(back_kernel, [((state_width, c), BF16)] * 2, [kept, befores], loads=(0,))
    others = turned(others, "seq_2", 1)
    pre, head, step_grad, kernels = call(
        back_through_kernel,
        [((t, c + mixed), F32), ((8, c + mixed), F32), ((t, 128), BF16), ((4, c + mixed), F32)],
        [
            who, mine, others, big, z, small, u, row_part, col_part, g, rate, skip, conv_inner,
            conv_mixer,
        ],
        loads=tuple(range(3, 14)),
        scratch=[pltpu.VMEM((state_width, c), BF16), pltpu.VMEM((state_width, c), BF16)],
        flops=500_000_000,
    )
    ahead = lax.ppermute(head, SEQ, [(k + 1, k) for k in range(seq_count - 1)])
    grads, mix_grads = call(
        conv_back_kernel,
        [((t, c + 128), BF16), ((t, mixed), BF16)],
        [pre, ahead, step_grad, kernels],
        scratch=[pltpu.VMEM((t + 8, c + mixed), F32)],
    )
    far, near, next_near = [turned(grads, ROW4, k) for k in (2, 1, 3)]
    same = [grads, near, far, next_near]
    shares = [turned(mix_grads, "chan", k) for k in (2, 1, 3)]
    (mix_total,) = call(add_kernel, [((t, mixed), BF16)], [mix_grads, *shares])
    far, near, next_near = [turned(mix_total, ROW4, k) for k in (2, 1, 3)]
    mix_same = [mix_total, near, far, next_near]
    swapped = [turned(v, "seq_2", 1) for v in same]
    mix_swapped = [turned(v, "seq_2", 1) for v in mix_same]
    partial = call(
        input_grad_kernel,
        [((part, model), BF16)] * chans,
        [who, grads, mix_grads, inner_weight, mixer_weight, step_weight.T],
        loads=(3, 4, 5),
        scratch=[pltpu.VMEM((tokens, model), BF16)],
        flops=500_000_000,
    )
    partial = [partial[0]] + [turned(partial[k], "chan", k) for k in (2, 1, 3)]
    (input_grad,) = call(add_kernel, [((part, model), BF16)], partial)
    (inner_terms,) = call(
        inner_weight_kernel,
        [((lines * share, c + 128), BF16)],
        [*slabs, *[v for pair in zip(same, swapped) for v in pair]],
        flops=700_000_000,
    )
    (terms,) = call(
        mixer_weight_kernel,
        [((lines, share, c + 128), BF16)],
        [who, *slabs, *[v for pair in zip(mix_same, mix_swapped) for v in pair], inner_terms],
        flops=700_000_000,
    )
    norm = 1.0 / math.sqrt(tokens * seq_count * lax.axis_size("dp"))
    terms = a2a(terms, "seq_0")
    inner_weight_grad, mixer_weight_grad, step_weight_grad = call(
        lambda *refs: total_kernel(*refs, norm=norm),
        [((share, c), F32), ((share // chans, mixed), F32), ((heads, share), F32)],
        [terms],
        scratch=[pltpu.VMEM((share, c + 128), F32)],
    )
    return input_grad[None], inner_weight_grad, mixer_weight_grad, step_weight_grad.T


def solution(mesh):
    split = Mesh(
        mesh.devices.reshape(mesh.shape["dp"], 8, 2, 2, mesh.shape["chan"]),
        ("dp", "seq_0", "seq_1", "seq_2", "chan"),
    )
    placed = (
        P("dp", SEQ_CHAN, None),
        P(None, "chan"),
        P(),
        P(None, "chan"),
        P(None, "chan"),
        P(),
        P("chan"),
        P("chan"),
        P("chan"),
        P("dp", SEQ, "chan"),
    )
    return jax.shard_map(
        layer,
        mesh=split,
        in_specs=placed,
        out_specs=(
            P("dp", SEQ_CHAN, None),
            P(DP_SEQ, "chan"),
            P(DP_SEQ_CHAN, None),
            P(DP_SEQ, "chan"),
        ),
        check_vma=False,
    )
```

```python
import math

import jax
import jax.numpy as jnp
from jax import lax
from jax.experimental import pallas as pl
from jax.experimental.pallas import tpu as pltpu
from jax.sharding import Mesh
from jax.sharding import PartitionSpec as P


HDIM = 64
SEQ = ("seq_0", "seq_1", "seq_2")
PAIRS = ("seq_0", "seq_1")
ROW4 = ("dp", "seq_1")
DP_SEQ = ("dp", "seq_0", "seq_1", "seq_2")
SEQ_CHAN = ("seq_0", "seq_1", "seq_2", "chan")
DP_SEQ_CHAN = ("dp", "seq_0", "seq_1", "seq_2", "chan")

F32 = jnp.float32
BF16 = jnp.bfloat16
HIGHEST = lax.Precision.HIGHEST
HALO = 16


def dot(a, b, ca=1, cb=0, precision=None):
    return lax.dot_general(
        a, b, (((ca,), (cb,)), ((), ())), precision=precision, preferred_element_type=F32
    )


def in_hbm(value):
    return pltpu.with_memory_space_constraint(value, pltpu.HBM)


def call(kernel, outs, ins, loads=(), stores=(), far=(), scratch=(), flops=0, early=False):
    count = len(ins)

    def wrapped(*refs):
        refs = list(refs)
        operands, results = refs[:count], refs[count : count + len(outs)]
        spare = refs[count + len(outs) :]
        sems = spare.pop()
        copies = []
        for k, position in enumerate(loads):
            buffer = spare.pop(0)
            copies.append(pltpu.make_async_copy(operands[position], buffer, sems.at[k]))
            operands[position] = buffer
        for copy in copies:
            copy.start()
        pending = {}
        for k, position in enumerate(stores):
            buffer = spare.pop(0)
            pending[position] = pltpu.make_async_copy(
                buffer, results[position], sems.at[len(loads) + k]
            )
            results[position] = buffer
        for copy in copies:
            copy.wait()
        started = []

        def flush(position):
            pending[position].start()
            started.append(position)

        if early:
            kernel(*operands, *results, *spare, flush=flush)
        else:
            kernel(*operands, *results, *spare)
        for position in stores:
            if position not in started:
                pending[position].start()
        for position in stores:
            pending[position].wait()

    specs, values = [], []
    for k, a in enumerate(ins):
        space = pltpu.VMEM
        if a.dtype == jnp.int32:
            space = pltpu.SMEM
        elif k in loads or k in far:
            space = pltpu.HBM
            a = in_hbm(a)
        specs.append(pl.BlockSpec(memory_space=space))
        values.append(a)
    buffers = [pltpu.VMEM(ins[k].shape, ins[k].dtype) for k in loads]
    buffers += [pltpu.VMEM(*outs[k]) for k in stores]
    return pl.pallas_call(
            wrapped,
            out_shape=[
                pltpu.HBM(s, d) if k in stores else jax.ShapeDtypeStruct(s, d)
                for k, (s, d) in enumerate(outs)
            ],
            in_specs=specs,
            out_specs=[
                pl.BlockSpec(memory_space=pltpu.HBM if k in stores else pltpu.VMEM)
                for k in range(len(outs))
            ],
            scratch_shapes=buffers
            + list(scratch)
            + [pltpu.SemaphoreType.DMA((len(loads) + len(stores) + 1,))],
            compiler_params=pltpu.CompilerParams(vmem_limit_bytes=24 << 20),
            cost_estimate=pl.CostEstimate(flops=flops, transcendentals=0, bytes_accessed=1 << 20),
    )(*values)


def fetch(values, after=None):
    count = len(values)

    def kernel(*refs):
        sources, outs, sems = refs[:count], refs[-1 - count : -1], refs[-1]
        copies = [
            pltpu.make_async_copy(source, out, sems.at[k])
            for k, (source, out) in enumerate(zip(sources, outs))
        ]
        for copy in copies:
            copy.start()
        for copy in copies:
            copy.wait()

    extra = [] if after is None else [after]
    return pl.pallas_call(
        kernel,
        out_shape=[jax.ShapeDtypeStruct(v.shape, v.dtype) for v in values],
        in_specs=[pl.BlockSpec(memory_space=pltpu.HBM)] * count
        + [pl.BlockSpec(memory_space=pltpu.VMEM)] * len(extra),
        out_specs=[pl.BlockSpec(memory_space=pltpu.VMEM)] * count,
        scratch_shapes=[pltpu.SemaphoreType.DMA((count,))],
        compiler_params=pltpu.CompilerParams(vmem_limit_bytes=16 << 20),
        cost_estimate=pl.CostEstimate(flops=700_000_000, transcendentals=0, bytes_accessed=4 << 20),
    )(*[in_hbm(v) for v in values], *extra)


def heads_to_lanes(heads, width):
    head = lax.broadcasted_iota(jnp.int32, (heads, width), 0)
    lane = lax.broadcasted_iota(jnp.int32, (heads, width), 1)
    return (lane // HDIM == head).astype(F32)


def lanes_to_heads(width, heads):
    lane = lax.broadcasted_iota(jnp.int32, (width, heads), 0)
    head = lax.broadcasted_iota(jnp.int32, (width, heads), 1)
    return (lane // HDIM == head).astype(F32)


def lower(size):
    row = lax.broadcasted_iota(jnp.int32, (size, size), 0)
    col = lax.broadcasted_iota(jnp.int32, (size, size), 1)
    return row >= col


def silu_and_slope(v):
    gate = 1.0 / (1.0 + jnp.exp(-v))
    return v * gate, gate * (1.0 + v * (1.0 - gate))


def project_kernel(
    who, x0, x1, x2, x3, h0, h1, h2, h3, w_in, w_mix, w_step, k_in, k_mix, bias, decay_log, g,
    x_out, big, z_out, small, rows, keep, send, kept,
    xs, pi, pm, *, flush,
):
    chan, core = who[0], who[1]
    part = x0.shape[0]
    tokens = 4 * part
    width = k_in.shape[1]
    mixed = k_mix.shape[1]
    state_width = mixed // 2
    heads = bias.shape[1]
    for k, x in enumerate((x0, x1, x2, x3)):
        slot = lax.rem(chan + 4 - k, 4)
        xs[pl.ds(pl.multiple_of(HALO + slot * part, 16), part), :] = x[...]
    edge = h0.shape[0]
    xs[0:HALO, :] = jnp.zeros_like(xs[0:HALO, :])
    xs[0:edge, :] = h0[...] + h1[...] + h2[...] + h3[...]
    everything = xs[...]
    x_out[...] = xs[HALO:, :]
    flush(0)
    pi[...] = dot(everything, w_in[...]).astype(BF16).astype(F32)
    pm[...] = dot(everything, w_mix[...]).astype(BF16).astype(F32)
    pi[HALO - edge : HALO, :] = pi[0:edge, :]
    pm[HALO - edge : HALO, :] = pm[0:edge, :]
    raw = dot(xs[HALO:, :], w_step[...], 1, 1) + bias[...]

    def convolved(source, kernel):
        total = kernel[3:4, :] * source[HALO:, :]
        for k in range(3):
            start = HALO - 3 + k
            total = total + kernel[k : k + 1, :] * source[start : start + tokens, :]
        return total

    inner_act, inner_slope = silu_and_slope(convolved(pi, k_in))
    big[:, :width] = inner_act
    big[:, width : 2 * width] = inner_slope
    mix_act, mixer_slope = silu_and_slope(convolved(pm, k_mix))
    big[:, 2 * width : 2 * width + mixed] = mix_act
    big[:, 2 * width + mixed :] = mixer_slope
    flush(1)

    step = jnp.maximum(raw, 0.0) + jnp.log1p(jnp.exp(-jnp.abs(raw)))
    decay = -step * jnp.exp(decay_log[...])
    low = lower(tokens).astype(F32)
    total = dot(low, decay, precision=HIGHEST)
    rows[0] = dot(decay, low, 0, 1, precision=HIGHEST)
    row = lax.broadcasted_iota(jnp.int32, (tokens, tokens), 0)
    col = lax.broadcasted_iota(jnp.int32, (tokens, tokens), 1)
    rows[1] = dot(step, (row == col).astype(F32), 0, 0, precision=HIGHEST)
    last = total[tokens - 1 : tokens, :]
    ea = jnp.exp(total)
    tail = jnp.exp(last - total)
    small[0] = step
    small[1] = total
    small[2] = ea
    small[3] = tail
    small[4] = 1.0 / (1.0 + jnp.exp(-raw))
    spread = heads_to_lanes(heads, width)
    wide = dot(jnp.concatenate([tail * step, ea], axis=0), spread, precision=HIGHEST)
    zs = (wide[:tokens] * inner_act).astype(BF16)
    zg = (wide[tokens:] * g[...].astype(F32)).astype(BF16)
    z_out[:, :width] = zs
    z_out[:, width:] = zg
    for k in (2, 3, 4):
        flush(k)
    into = mix_act[:, :state_width].astype(BF16)
    out_of = mix_act[:, state_width:].astype(BF16)
    state = dot(into, zs, 0, 0)
    grad = dot(out_of, zg, 0, 0)
    lead = last.astype(BF16)
    keep[:, width:] = jnp.zeros_like(keep[:, width:])
    send[:, width:] = jnp.zeros_like(send[:, width:])
    keep[0:1, width : width + heads] = last
    send[0:1, width : width + heads] = lead
    send[1:2, width : width + heads] = (last - lead.astype(F32)).astype(BF16)

    @pl.when(core == 0)
    def _():
        keep[:, :width] = state
        send[:, :width] = grad.astype(BF16)

    @pl.when(core != 0)
    def _():
        keep[:, :width] = grad
        send[:, :width] = state.astype(BF16)

    kept[...] = keep[...]


def pair_kernel(keep, recv, out):
    groups, per = out.shape[0], out.shape[1]
    heads = out.shape[2] // HDIM - 2
    width = heads * HDIM
    spread = heads_to_lanes(heads, width)
    own = keep[0:8, width : width + heads]
    other = recv[0:16, width : width + heads].astype(F32)
    theirs = other[0:1] + other[1:2]
    wide = dot(jnp.broadcast_to(jnp.exp(theirs), (8, heads)), spread, precision=HIGHEST)
    pair = (wide[0:1] * keep[:, :width] + recv[:, :width].astype(F32)).astype(BF16)
    total = own[0:1] + theirs
    lead = total.astype(BF16)
    rest = (total - lead.astype(F32)).astype(BF16)
    out[:, :, :width] = pair.reshape(groups, per, width)
    out[:, :, width:] = jnp.zeros_like(out[:, :, width:])
    for k in range(groups):
        out[k, 0:1, width : width + heads] = lead
        out[k, 1:2, width : width + heads] = rest


def chain_kernel(who, recv, out, factors):
    forward = who[1] == 0
    groups = recv.shape[0]
    width = out.shape[2]
    heads = width // HDIM
    marks = recv[:, 0, width : width + heads].astype(F32)
    marks = marks + recv[:, 1, width : width + heads].astype(F32)
    factors[...] = dot(jnp.exp(marks), heads_to_lanes(heads, width), precision=HIGHEST)

    def step(k, state):
        slot = jnp.where(forward, k, groups - 1 - k)
        out[slot] = state.astype(BF16)
        return factors[pl.ds(slot, 1), :] * state + recv[slot, :, :width].astype(F32)

    lax.fori_loop(0, groups, step, jnp.zeros(out.shape[1:], F32), unroll=True)


def back_kernel(keep, before, own, send):
    groups, per, width = before.shape
    heads = width // HDIM
    last = jnp.broadcast_to(keep[0:1, width : width + heads], (8, heads))
    factor = dot(jnp.exp(last), heads_to_lanes(heads, width), precision=HIGHEST)[0:1]
    piece = before[...].reshape(groups * per, width)
    own[...] = piece
    send[...] = (factor * piece.astype(F32) + keep[:, :width]).astype(BF16)


def pack_kernel(who, x, keep, send, turned_x, *, half):
    core, place = who[1], who[2]
    model = x.shape[1]
    lines = 8
    share = keep.shape[1] // lines
    for k in range(model // 128):
        lanes = slice(k * 128, (k + 1) * 128)
        turned_x[lanes, :] = x[:, lanes].astype(F32).T
    for out, side in ((keep, core), (send, 1 - core)):
        for steps in range(4):
            where = lax.rem(place + steps, 4)
            outer = where // half
            inner = 2 * (where - outer * half) + side
            for line in range(lines):
                start = share * ((outer * lines + line) * 2 * half + inner)
                out[steps, line * share : (line + 1) * share, :] = turned_x[
                    pl.ds(pl.multiple_of(start, 8), share), :
                ].astype(BF16)


def join_kernel(keep, got, *outs):
    for k, out in enumerate(outs):
        out[0] = keep[k]
        out[1] = got[k]


def within_kernel(big, g, small, rows, u_out, row_out, col_out):
    tokens, width = g.shape
    mixed = (big.shape[1] - 2 * width) // 2
    state_width = mixed // 2
    into = big[:, 2 * width : 2 * width + state_width].astype(BF16)
    out_of = big[:, 2 * width + state_width : 2 * width + mixed].astype(BF16)
    scores = dot(out_of, into, 1, 1)
    causal = lower(tokens)
    lane = lax.broadcasted_iota(jnp.int32, (tokens, 128), 1)
    pull = jnp.zeros((tokens, tokens), F32)
    for pair in range(width // 128):
        lanes = slice(pair * 128, (pair + 1) * 128)
        x_pair = big[:, lanes].astype(BF16)
        g_pair = g[:, lanes]
        u_pair = jnp.zeros((tokens, 128), F32)
        for half in range(2):
            h = 2 * pair + half
            g_head = jnp.where(lane // HDIM == half, g_pair, jnp.zeros_like(g_pair))
            inner = dot(g_head, x_pair, 1, 1)
            spread = small[1, :, h : h + 1] - rows[0, h : h + 1, :]
            decay = jnp.where(causal, jnp.exp(jnp.where(causal, spread, 0.0)), 0.0)
            weights = decay * scores
            u_pair = u_pair + dot(weights.astype(BF16), g_head, 0, 0)
            step_row = rows[1, h : h + 1, :]
            both = weights * inner
            col_out[h : h + 1, :] = jnp.sum(both, axis=0, keepdims=True)
            row_out[:, h : h + 1] = jnp.sum(both * step_row, axis=1, keepdims=True)
            pull = pull + decay * inner * step_row
        u_out[:, lanes] = u_pair
    pull = pull.astype(BF16)
    u_out[:, width : width + state_width] = dot(pull, out_of, 0, 0)
    u_out[:, width + state_width :] = dot(pull, into)


def back_through_kernel(
    who, own, other, big, z, small, u, row_in, col_in, g, decay_log, skip, k_in, k_mix,
    pre_out, head_out, step_out, k_out, s0, gt,
):
    tokens, width = g.shape
    heads = small.shape[2]
    mixed = (big.shape[1] - 2 * width) // 2
    state_width = mixed // 2

    @pl.when(who[1] == 0)
    def _():
        s0[...] = own[...]
        gt[...] = other[...]

    @pl.when(who[1] != 0)
    def _():
        s0[...] = other[...]
        gt[...] = own[...]

    into = big[:, 2 * width : 2 * width + state_width].astype(BF16)
    out_of = big[:, 2 * width + state_width : 2 * width + mixed].astype(BF16)
    zs = z[:, :width]
    zg = z[:, width:]
    gb = dot(into, gt[...])
    sc = dot(out_of, s0[...])
    step = small[0]
    spread = heads_to_lanes(heads, width)
    gather = lanes_to_heads(width, heads)
    skip_rows = jnp.broadcast_to(skip[...], (8, heads))
    wide = dot(
        jnp.concatenate([step, small[3], skip_rows], axis=0), spread, precision=HIGHEST
    )
    tail_gb = wide[tokens : 2 * tokens] * gb
    x = big[:, :width]
    upstream = g[...].astype(F32)
    d_act = wide[:tokens] * (u[:, :width] + tail_gb) + wide[2 * tokens : 2 * tokens + 1] * upstream
    d_pre = d_act * big[:, width : 2 * width]
    pre_out[:, :width] = d_pre
    cross = jnp.sum(gt[...].astype(F32) * s0[...].astype(F32), axis=0, keepdims=True)
    sums = dot(
        jnp.concatenate(
            [x * tail_gb, zg.astype(F32) * sc, jnp.broadcast_to(cross, (8, width))], axis=0
        ),
        gather,
        precision=HIGHEST,
    )
    e_part = sums[:tokens]
    c_part = sums[tokens : 2 * tokens]
    f_part = sums[2 * tokens : 2 * tokens + 1]
    row = lax.broadcasted_iota(jnp.int32, (tokens, tokens), 0)
    col = lax.broadcasted_iota(jnp.int32, (tokens, tokens), 1)
    col_part = dot((row == col).astype(F32), col_in[...], 1, 1, precision=HIGHEST)
    e_step = step * e_part
    d_total = row_in[...] + c_part - step * col_part - e_step
    at_end = jnp.sum(e_step, axis=0, keepdims=True) + small[2, tokens - 1 : tokens, :] * f_part
    d_decay = dot((row <= col).astype(F32), d_total, precision=HIGHEST) + at_end
    d_step = col_part + e_part - d_decay * jnp.exp(decay_log[...])
    step_out[...] = jnp.zeros_like(step_out)
    step_out[:, :heads] = (d_step * small[4]).astype(BF16)
    d_into = u[:, width : width + state_width] + dot(zs, gt[...], 1, 1)
    d_out_of = u[:, width + state_width :] + dot(zg, s0[...], 1, 1)
    slopes = 2 * width + mixed
    pre_out[:, width : width + state_width] = d_into * big[:, slopes : slopes + state_width]
    pre_out[:, width + state_width :] = d_out_of * big[:, slopes + state_width :]
    head_out[...] = pre_out[0:8, :]
    k_out[:, :width] = k_in[...]
    k_out[:, width:] = k_mix[...]


def conv_back_kernel(pre, ahead, step, kernel, out, mix_out, padded):
    tokens = pre.shape[0]
    width = out.shape[1] - 128
    padded[:tokens, :] = pre[...]
    padded[tokens:, :] = ahead[...]

    def convolved(lanes):
        total = kernel[3:4, lanes] * padded[:tokens, lanes]
        for k in range(3):
            total = total + kernel[k : k + 1, lanes] * padded[3 - k : 3 - k + tokens, lanes]
        return total

    out[:, :width] = convolved(slice(0, width)).astype(BF16)
    out[:, width:] = step[...]
    mix_out[...] = convolved(slice(width, pre.shape[1])).astype(BF16)


def input_grad_kernel(who, grads, mix_grads, w_mix, w_step, w_in, *refs):
    outs, whole = refs[:4], refs[4]
    width = w_in.shape[1]
    heads = w_step.shape[0]
    total = dot(grads[:, :width], w_in[...], 1, 1)
    total = total + dot(mix_grads[...], w_mix[...], 1, 1)
    total = total + dot(grads[:, width : width + heads], w_step[...])
    whole[...] = total.astype(BF16)
    part = outs[0].shape[0]
    for k, out in enumerate(outs):
        slot = lax.rem(who[0] + k, 4)
        out[...] = whole[pl.ds(pl.multiple_of(slot * part, 16), part), :]


def pair_add_kernel(a, b, out):
    out[...] = (a[...].astype(F32) + b[...].astype(F32)).astype(BF16)


def add_kernel(m0, m1, m2, m3, out):
    total = m0[...].astype(F32) + m1[...].astype(F32) + m2[...].astype(F32) + m3[...].astype(F32)
    out[...] = total.astype(BF16)


def gathered_product(slabs, grads):
    total = None
    for k, grad in enumerate(grads):
        part = dot(slabs[k // 2][k % 2], grad[...])
        total = part if total is None else total + part
    return total


def inner_weight_kernel(*refs):
    refs[-1][...] = gathered_product(refs[:4], refs[4:12]).astype(BF16)


def mixer_weight_kernel(who, *refs):
    slabs, grads, inner, out = refs[:4], refs[4:12], refs[12], refs[13]
    chan = who[0]
    lines, share, _ = out.shape
    total = gathered_product(slabs, grads).astype(BF16)
    few = share // 4
    to_row = lax.broadcasted_iota(jnp.int32, (share, 4 * share), 0)
    source = lax.broadcasted_iota(jnp.int32, (share, 4 * share), 1)
    group = to_row // few
    wanted = group * share + chan * few + (to_row - group * few)
    pick = (source == wanted).astype(BF16)
    edge = inner.shape[1] - 64
    out[:, :, :] = inner[...].reshape(out.shape)
    for line in range(lines):
        piece = total[line * share : (line + 1) * share, :]
        stacked = jnp.concatenate([piece[:, q * 64 : (q + 1) * 64] for q in range(4)], axis=0)
        out[line, :, edge:] = dot(pick, stacked).astype(BF16)


def total_kernel(terms, inner_out, mix_out, step_out, whole, *, norm):
    lines, share, _ = terms.shape
    width = inner_out.shape[1]
    few = share // 4
    total = terms[0].astype(F32)
    for k in range(1, lines):
        total = total + terms[k].astype(F32)
    whole[...] = total * norm
    inner_out[...] = whole[:, :width]
    edge = whole.shape[1] - 64
    for q in range(4):
        mix_out[:, q * 64 : (q + 1) * 64] = whole[q * few : (q + 1) * few, edge:]
    heads = step_out.shape[0]
    row = lax.broadcasted_iota(jnp.int32, (heads, 128), 0)
    col = lax.broadcasted_iota(jnp.int32, (heads, 128), 1)
    step_out[...] = dot(
        (row == col).astype(F32), whole[:, width : width + 128], 1, 1, precision=HIGHEST
    )


def a2a(value, axis):
    return lax.all_to_all(value, axis, split_axis=0, concat_axis=0, tiled=True)


def turned(value, axis, steps):
    count = lax.axis_size(axis)
    return lax.ppermute(value, axis, [(k, (k + steps) % count) for k in range(count)])


def layer(
    layer_input,
    inner_weight,
    mixer_weight,
    step_weight,
    conv_inner,
    conv_mixer,
    step_bias,
    decay_log,
    skip_gain,
    output_grad,
):
    own = layer_input[0]
    part, model = own.shape
    chans = lax.axis_size("chan")
    tokens = part * chans
    width = inner_weight.shape[1]
    heads = step_bias.shape[0]
    mixed = mixer_weight.shape[1]
    state_width = mixed // 2
    g = output_grad[0]
    who = jnp.stack(
        [lax.axis_index("chan"), lax.axis_index("seq_2"), lax.axis_index(ROW4)]
    ).astype(jnp.int32)
    bias = step_bias[None]
    rate = decay_log[None]
    skip = skip_gain[None]

    seq_count = lax.axis_size(SEQ)
    t, c = tokens, width

    arrived = [turned(own, "chan", k) for k in (1, 2, 3)]
    tail_rows = own[part - 4 :]
    halos = [
        lax.ppermute(
            tail_rows,
            SEQ_CHAN,
            [(s * chans + chans - 1, (s + 1) * chans + k) for s in range(seq_count - 1)],
        )
        for k in range(chans)
    ]
    sources = [
        own, inner_weight, mixer_weight, step_weight.T, conv_inner, conv_mixer, bias, rate, g
    ]
    near = fetch(sources)
    x, big, z, small, rows, keep, send, kept = call(
        project_kernel,
        [
            ((t, model), BF16),
            ((t, 2 * c + 2 * mixed), F32),
            ((t, 2 * c), BF16),
            ((5, t, heads), F32),
            ((2, heads, t), F32),
            ((state_width, c + 128), F32),
            ((state_width, c + 128), BF16),
            ((state_width, c + 128), F32),
        ],
        [who, near[0], *arrived, *halos, *near[1:]],
        stores=(0, 1, 2, 3, 4, 7),
        scratch=[
            pltpu.VMEM((t + HALO, model), BF16),
            pltpu.VMEM((t + HALO, c), F32),
            pltpu.VMEM((t + HALO, mixed), F32),
        ],
        flops=700_000_000,
        early=True,
    )
    got = turned(send, "seq_2", 1)
    groups = lax.axis_size(PAIRS)
    per = state_width // groups
    (pairs,) = call(pair_kernel, [((groups, per, c + 128), BF16)], [keep, got])
    pairs = a2a(pairs, PAIRS)

    u, row_part, col_part = call(
        within_kernel,
        [((t, c + mixed), F32), ((t, heads), F32), ((heads, t), F32)],
        [big, g, small, rows],
        loads=(0, 1, 2, 3),
        stores=(0, 1, 2),
        flops=700_000_000,
    )
    share = model // lax.axis_size(DP_SEQ)
    lines = lax.axis_size("seq_0")
    slab_shape = (lines * share, t)
    slab_keep, slab_send = call(
        lambda *refs: pack_kernel(*refs, half=lax.axis_size("seq_1")),
        [((4, *slab_shape), BF16)] * 2,
        [who, x],
        loads=(1,),
        stores=(0, 1),
        scratch=[pltpu.VMEM((model, t), F32)],
        flops=500_000_000,
    )
    slab_got = turned(slab_send, "seq_2", 1)
    slabs = call(
        join_kernel,
        [((2, *slab_shape), BF16)] * 4,
        [slab_keep, slab_got],
        loads=(0,),
        stores=(0,),
        flops=500_000_000,
    )
    far, close, next_close = [turned(slabs[k], ROW4, k) for k in (2, 1, 3)]
    slabs = [slabs[0], close, far, next_close]

    (befores,) = call(
        chain_kernel,
        [((groups, per, c), BF16)],
        [who, pairs],
        scratch=[pltpu.VMEM((groups, c), F32)],
    )
    befores = a2a(befores, PAIRS)
    mine, others = call(back_kernel, [((state_width, c), BF16)] * 2, [kept, befores], loads=(0,))
    others = turned(others, "seq_2", 1)
    sources = [big, z, small, u, row_part, col_part, g, rate, skip, conv_inner, conv_mixer]
    fetched = fetch(sources, after=mine)
    pre, head, step_grad, kernels = call(
        back_through_kernel,
        [((t, c + mixed), F32), ((8, c + mixed), F32), ((t, 128), BF16), ((4, c + mixed), F32)],
        [who, mine, others, *fetched],
        scratch=[pltpu.VMEM((state_width, c), BF16), pltpu.VMEM((state_width, c), BF16)],
        flops=500_000_000,
    )
    ahead = lax.ppermute(head, SEQ, [(k + 1, k) for k in range(seq_count - 1)])
    grads, mix_grads = call(
        conv_back_kernel,
        [((t, c + 128), BF16), ((t, mixed), BF16)],
        [pre, ahead, step_grad, kernels],
        scratch=[pltpu.VMEM((t + 8, c + mixed), F32)],
    )
    far, near, next_near = [turned(grads, ROW4, k) for k in (2, 1, 3)]
    same = [grads, near, far, next_near]
    mix_total = mix_grads
    for partners in ([1, 0, 3, 2], [3, 2, 1, 0]):
        theirs = lax.ppermute(mix_total, "chan", list(enumerate(partners)))
        (mix_total,) = call(pair_add_kernel, [((t, mixed), BF16)], [mix_total, theirs])
    far, near, next_near = [turned(mix_total, ROW4, k) for k in (2, 1, 3)]
    mix_same = [mix_total, near, far, next_near]
    swapped = [turned(v, "seq_2", 1) for v in same]
    mix_swapped = [turned(v, "seq_2", 1) for v in mix_same]
    partial = call(
        input_grad_kernel,
        [((part, model), BF16)] * chans,
        [who, grads, mix_grads, mixer_weight, step_weight.T, inner_weight],
        stores=(0, 1, 2, 3),
        scratch=[pltpu.VMEM((tokens, model), BF16)],
        flops=500_000_000,
    )
    partial = [partial[0]] + [turned(partial[k], "chan", k) for k in (2, 1, 3)]
    (input_grad,) = call(add_kernel, [((part, model), BF16)], partial)
    (inner_terms,) = call(
        inner_weight_kernel,
        [((lines * share, c + 128), BF16)],
        [*slabs, *[v for pair in zip(same, swapped) for v in pair]],
        flops=700_000_000,
    )
    (terms,) = call(
        mixer_weight_kernel,
        [((lines, share, c + 128), BF16)],
        [who, *slabs, *[v for pair in zip(mix_same, mix_swapped) for v in pair], inner_terms],
        flops=700_000_000,
    )
    norm = 1.0 / math.sqrt(tokens * seq_count * lax.axis_size("dp"))
    terms = a2a(terms, "seq_0")
    inner_weight_grad, mixer_weight_grad, step_weight_grad = call(
        lambda *refs: total_kernel(*refs, norm=norm),
        [((share, c), F32), ((share // chans, mixed), F32), ((heads, share), F32)],
        [terms],
        scratch=[pltpu.VMEM((share, c + 128), F32)],
    )
    return input_grad[None], inner_weight_grad, mixer_weight_grad, step_weight_grad.T


def solution(mesh):
    split = Mesh(
        mesh.devices.reshape(mesh.shape["dp"], 8, 2, 2, mesh.shape["chan"]),
        ("dp", "seq_0", "seq_1", "seq_2", "chan"),
    )
    placed = (
        P("dp", SEQ_CHAN, None),
        P(None, "chan"),
        P(),
        P(None, "chan"),
        P(None, "chan"),
        P(),
        P("chan"),
        P("chan"),
        P("chan"),
        P("dp", SEQ, "chan"),
    )
    return jax.shard_map(
        layer,
        mesh=split,
        in_specs=placed,
        out_specs=(
            P("dp", SEQ_CHAN, None),
            P(DP_SEQ, "chan"),
            P(DP_SEQ_CHAN, None),
            P(DP_SEQ, "chan"),
        ),
        check_vma=False,
    )
```

```python
import math

import jax
import jax.numpy as jnp
from jax import lax
from jax.experimental import pallas as pl
from jax.experimental.pallas import tpu as pltpu
from jax.sharding import Mesh
from jax.sharding import PartitionSpec as P


HDIM = 64
SEQ = ("seq_0", "seq_1", "seq_2")
PAIRS = ("seq_0", "seq_1")
ROW4 = ("dp", "seq_1")
DP_SEQ = ("dp", "seq_0", "seq_1", "seq_2")
SEQ_CHAN = ("seq_0", "seq_1", "seq_2", "chan")
DP_SEQ_CHAN = ("dp", "seq_0", "seq_1", "seq_2", "chan")

F32 = jnp.float32
BF16 = jnp.bfloat16
HIGHEST = lax.Precision.HIGHEST
HALO = 16


def dot(a, b, ca=1, cb=0, precision=None):
    return lax.dot_general(
        a, b, (((ca,), (cb,)), ((), ())), precision=precision, preferred_element_type=F32
    )


def in_hbm(value):
    return pltpu.with_memory_space_constraint(value, pltpu.HBM)


def call(kernel, outs, ins, loads=(), stores=(), far=(), scratch=(), flops=0, early=False):
    count = len(ins)

    def wrapped(*refs):
        refs = list(refs)
        operands, results = refs[:count], refs[count : count + len(outs)]
        spare = refs[count + len(outs) :]
        sems = spare.pop()
        copies = []
        for k, position in enumerate(loads):
            buffer = spare.pop(0)
            copies.append(pltpu.make_async_copy(operands[position], buffer, sems.at[k]))
            operands[position] = buffer
        for copy in copies:
            copy.start()
        pending = {}
        for k, position in enumerate(stores):
            buffer = spare.pop(0)
            pending[position] = pltpu.make_async_copy(
                buffer, results[position], sems.at[len(loads) + k]
            )
            results[position] = buffer
        for copy in copies:
            copy.wait()
        started = []

        def flush(position):
            pending[position].start()
            started.append(position)

        if early:
            kernel(*operands, *results, *spare, flush=flush)
        else:
            kernel(*operands, *results, *spare)
        for position in stores:
            if position not in started:
                pending[position].start()
        for position in stores:
            pending[position].wait()

    specs, values = [], []
    for k, a in enumerate(ins):
        space = pltpu.VMEM
        if a.dtype == jnp.int32:
            space = pltpu.SMEM
        elif k in loads or k in far:
            space = pltpu.HBM
            a = in_hbm(a)
        specs.append(pl.BlockSpec(memory_space=space))
        values.append(a)
    buffers = [pltpu.VMEM(ins[k].shape, ins[k].dtype) for k in loads]
    buffers += [pltpu.VMEM(*outs[k]) for k in stores]
    return pl.pallas_call(
            wrapped,
            out_shape=[
                pltpu.HBM(s, d) if k in stores else jax.ShapeDtypeStruct(s, d)
                for k, (s, d) in enumerate(outs)
            ],
            in_specs=specs,
            out_specs=[
                pl.BlockSpec(memory_space=pltpu.HBM if k in stores else pltpu.VMEM)
                for k in range(len(outs))
            ],
            scratch_shapes=buffers
            + list(scratch)
            + [pltpu.SemaphoreType.DMA((len(loads) + len(stores) + 1,))],
            compiler_params=pltpu.CompilerParams(vmem_limit_bytes=24 << 20),
            cost_estimate=pl.CostEstimate(flops=flops, transcendentals=0, bytes_accessed=1 << 20),
    )(*values)


def fetch(values, after=None):
    count = len(values)

    def kernel(*refs):
        sources, outs, sems = refs[:count], refs[-1 - count : -1], refs[-1]
        copies = [
            pltpu.make_async_copy(source, out, sems.at[k])
            for k, (source, out) in enumerate(zip(sources, outs))
        ]
        for copy in copies:
            copy.start()
        for copy in copies:
            copy.wait()

    extra = [] if after is None else [after]
    return pl.pallas_call(
        kernel,
        out_shape=[jax.ShapeDtypeStruct(v.shape, v.dtype) for v in values],
        in_specs=[pl.BlockSpec(memory_space=pltpu.HBM)] * count
        + [pl.BlockSpec(memory_space=pltpu.VMEM)] * len(extra),
        out_specs=[pl.BlockSpec(memory_space=pltpu.VMEM)] * count,
        scratch_shapes=[pltpu.SemaphoreType.DMA((count,))],
        compiler_params=pltpu.CompilerParams(vmem_limit_bytes=16 << 20),
        cost_estimate=pl.CostEstimate(flops=700_000_000, transcendentals=0, bytes_accessed=4 << 20),
    )(*[in_hbm(v) for v in values], *extra)


def heads_to_lanes(heads, width):
    head = lax.broadcasted_iota(jnp.int32, (heads, width), 0)
    lane = lax.broadcasted_iota(jnp.int32, (heads, width), 1)
    return (lane // HDIM == head).astype(F32)


def lanes_to_heads(width, heads):
    lane = lax.broadcasted_iota(jnp.int32, (width, heads), 0)
    head = lax.broadcasted_iota(jnp.int32, (width, heads), 1)
    return (lane // HDIM == head).astype(F32)


def lower(size):
    row = lax.broadcasted_iota(jnp.int32, (size, size), 0)
    col = lax.broadcasted_iota(jnp.int32, (size, size), 1)
    return row >= col


def silu_and_slope(v):
    gate = 1.0 / (1.0 + jnp.exp(-v))
    return v * gate, gate * (1.0 + v * (1.0 - gate))


def project_kernel(
    who, x0, x1, x2, x3, h0, h1, h2, h3, w_in, w_mix, w_step, k_in, k_mix, bias, decay_log, g,
    x_out, big, z_out, small, rows, keep, send, kept,
    xs, pi, pm, *, flush,
):
    chan, core = who[0], who[1]
    part = x0.shape[0]
    tokens = 4 * part
    width = k_in.shape[1]
    mixed = k_mix.shape[1]
    state_width = mixed // 2
    heads = bias.shape[1]
    for k, x in enumerate((x0, x1, x2, x3)):
        slot = lax.rem(chan + 4 - k, 4)
        xs[pl.ds(pl.multiple_of(HALO + slot * part, 16), part), :] = x[...]
    edge = h0.shape[0]
    xs[0:HALO, :] = jnp.zeros_like(xs[0:HALO, :])
    xs[0:edge, :] = h0[...] + h1[...] + h2[...] + h3[...]
    everything = xs[...]
    x_out[...] = xs[HALO:, :]
    flush(0)
    pi[...] = dot(everything, w_in[...]).astype(BF16).astype(F32)
    pm[...] = dot(everything, w_mix[...]).astype(BF16).astype(F32)
    pi[HALO - edge : HALO, :] = pi[0:edge, :]
    pm[HALO - edge : HALO, :] = pm[0:edge, :]
    raw = dot(xs[HALO:, :], w_step[...], 1, 1) + bias[...]

    def convolved(source, kernel):
        total = kernel[3:4, :] * source[HALO:, :]
        for k in range(3):
            start = HALO - 3 + k
            total = total + kernel[k : k + 1, :] * source[start : start + tokens, :]
        return total

    inner_act, inner_slope = silu_and_slope(convolved(pi, k_in))
    big[:, :width] = inner_act
    big[:, width : 2 * width] = inner_slope
    mix_act, mixer_slope = silu_and_slope(convolved(pm, k_mix))
    big[:, 2 * width : 2 * width + mixed] = mix_act
    big[:, 2 * width + mixed :] = mixer_slope
    flush(1)

    step = jnp.maximum(raw, 0.0) + jnp.log1p(jnp.exp(-jnp.abs(raw)))
    decay = -step * jnp.exp(decay_log[...])
    low = lower(tokens).astype(F32)
    total = dot(low, decay, precision=HIGHEST)
    rows[0] = dot(decay, low, 0, 1, precision=HIGHEST)
    row = lax.broadcasted_iota(jnp.int32, (tokens, tokens), 0)
    col = lax.broadcasted_iota(jnp.int32, (tokens, tokens), 1)
    rows[1] = dot(step, (row == col).astype(F32), 0, 0, precision=HIGHEST)
    last = total[tokens - 1 : tokens, :]
    ea = jnp.exp(total)
    tail = jnp.exp(last - total)
    small[0] = step
    small[1] = total
    small[2] = ea
    small[3] = tail
    small[4] = 1.0 / (1.0 + jnp.exp(-raw))
    spread = heads_to_lanes(heads, width)
    wide = dot(jnp.concatenate([tail * step, ea], axis=0), spread, precision=HIGHEST)
    zs = (wide[:tokens] * inner_act).astype(BF16)
    zg = (wide[tokens:] * g[...].astype(F32)).astype(BF16)
    z_out[:, :width] = zs
    z_out[:, width:] = zg
    for k in (2, 3, 4):
        flush(k)
    into = mix_act[:, :state_width].astype(BF16)
    out_of = mix_act[:, state_width:].astype(BF16)
    state = dot(into, zs, 0, 0)
    grad = dot(out_of, zg, 0, 0)
    lead = last.astype(BF16)
    keep[:, width:] = jnp.zeros_like(keep[:, width:])
    send[:, width:] = jnp.zeros_like(send[:, width:])
    keep[0:1, width : width + heads] = last
    send[0:1, width : width + heads] = lead
    send[1:2, width : width + heads] = (last - lead.astype(F32)).astype(BF16)

    @pl.when(core == 0)
    def _():
        keep[:, :width] = state
        send[:, :width] = grad.astype(BF16)

    @pl.when(core != 0)
    def _():
        keep[:, :width] = grad
        send[:, :width] = state.astype(BF16)

    kept[...] = keep[...]


def pair_kernel(keep, recv, out):
    groups, per = out.shape[0], out.shape[1]
    heads = out.shape[2] // HDIM - 2
    width = heads * HDIM
    spread = heads_to_lanes(heads, width)
    own = keep[0:8, width : width + heads]
    other = recv[0:16, width : width + heads].astype(F32)
    theirs = other[0:1] + other[1:2]
    wide = dot(jnp.broadcast_to(jnp.exp(theirs), (8, heads)), spread, precision=HIGHEST)
    pair = (wide[0:1] * keep[:, :width] + recv[:, :width].astype(F32)).astype(BF16)
    total = own[0:1] + theirs
    lead = total.astype(BF16)
    rest = (total - lead.astype(F32)).astype(BF16)
    out[:, :, :width] = pair.reshape(groups, per, width)
    out[:, :, width:] = jnp.zeros_like(out[:, :, width:])
    for k in range(groups):
        out[k, 0:1, width : width + heads] = lead
        out[k, 1:2, width : width + heads] = rest


def chain_kernel(who, recv, out, factors):
    forward = who[1] == 0
    groups = recv.shape[0]
    width = out.shape[2]
    heads = width // HDIM
    marks = recv[:, 0, width : width + heads].astype(F32)
    marks = marks + recv[:, 1, width : width + heads].astype(F32)
    factors[...] = dot(jnp.exp(marks), heads_to_lanes(heads, width), precision=HIGHEST)

    def step(k, state):
        slot = jnp.where(forward, k, groups - 1 - k)
        out[slot] = state.astype(BF16)
        return factors[pl.ds(slot, 1), :] * state + recv[slot, :, :width].astype(F32)

    lax.fori_loop(0, groups, step, jnp.zeros(out.shape[1:], F32), unroll=True)


def back_kernel(keep, before, own, send):
    groups, per, width = before.shape
    heads = width // HDIM
    last = jnp.broadcast_to(keep[0:1, width : width + heads], (8, heads))
    factor = dot(jnp.exp(last), heads_to_lanes(heads, width), precision=HIGHEST)[0:1]
    piece = before[...].reshape(groups * per, width)
    own[...] = piece
    send[...] = (factor * piece.astype(F32) + keep[:, :width]).astype(BF16)


def pack_kernel(who, x, keep, send, turned_x, *, half):
    core, place = who[1], who[2]
    model = x.shape[1]
    lines = 8
    share = keep.shape[1] // lines
    for k in range(model // 128):
        lanes = slice(k * 128, (k + 1) * 128)
        turned_x[lanes, :] = x[:, lanes].astype(F32).T
    for out, side in ((keep, core), (send, 1 - core)):
        for steps in range(4):
            where = lax.rem(place + steps, 4)
            outer = where // half
            inner = 2 * (where - outer * half) + side
            for line in range(lines):
                start = share * ((outer * lines + line) * 2 * half + inner)
                out[steps, line * share : (line + 1) * share, :] = turned_x[
                    pl.ds(pl.multiple_of(start, 8), share), :
                ].astype(BF16)


def join_kernel(keep, got, *outs):
    for k, out in enumerate(outs):
        out[0] = keep[k]
        out[1] = got[k]


def within_kernel(big, g, small, rows, u_out, row_out, col_out):
    tokens, width = g.shape
    mixed = (big.shape[1] - 2 * width) // 2
    state_width = mixed // 2
    into = big[:, 2 * width : 2 * width + state_width].astype(BF16)
    out_of = big[:, 2 * width + state_width : 2 * width + mixed].astype(BF16)
    scores = dot(out_of, into, 1, 1)
    causal = lower(tokens)
    lane = lax.broadcasted_iota(jnp.int32, (tokens, 128), 1)
    pull = jnp.zeros((tokens, tokens), F32)
    for pair in range(width // 128):
        lanes = slice(pair * 128, (pair + 1) * 128)
        x_pair = big[:, lanes].astype(BF16)
        g_pair = g[:, lanes]
        u_pair = jnp.zeros((tokens, 128), F32)
        for half in range(2):
            h = 2 * pair + half
            g_head = jnp.where(lane // HDIM == half, g_pair, jnp.zeros_like(g_pair))
            inner = dot(g_head, x_pair, 1, 1)
            spread = small[1, :, h : h + 1] - rows[0, h : h + 1, :]
            decay = jnp.where(causal, jnp.exp(jnp.where(causal, spread, 0.0)), 0.0)
            weights = decay * scores
            u_pair = u_pair + dot(weights.astype(BF16), g_head, 0, 0)
            step_row = rows[1, h : h + 1, :]
            both = weights * inner
            col_out[h : h + 1, :] = jnp.sum(both, axis=0, keepdims=True)
            row_out[:, h : h + 1] = jnp.sum(both * step_row, axis=1, keepdims=True)
            pull = pull + decay * inner * step_row
        u_out[:, lanes] = u_pair
    pull = pull.astype(BF16)
    u_out[:, width : width + state_width] = dot(pull, out_of, 0, 0)
    u_out[:, width + state_width :] = dot(pull, into)


def back_through_kernel(
    who, own, other, big, z, small, u, row_in, col_in, g, decay_log, skip, k_in, k_mix,
    pre_out, head_out, step_out, k_out, s0, gt,
):
    tokens, width = g.shape
    heads = small.shape[2]
    mixed = (big.shape[1] - 2 * width) // 2
    state_width = mixed // 2

    @pl.when(who[1] == 0)
    def _():
        s0[...] = own[...]
        gt[...] = other[...]

    @pl.when(who[1] != 0)
    def _():
        s0[...] = other[...]
        gt[...] = own[...]

    into = big[:, 2 * width : 2 * width + state_width].astype(BF16)
    out_of = big[:, 2 * width + state_width : 2 * width + mixed].astype(BF16)
    zs = z[:, :width]
    zg = z[:, width:]
    gb = dot(into, gt[...])
    sc = dot(out_of, s0[...])
    step = small[0]
    spread = heads_to_lanes(heads, width)
    gather = lanes_to_heads(width, heads)
    skip_rows = jnp.broadcast_to(skip[...], (8, heads))
    wide = dot(
        jnp.concatenate([step, small[3], skip_rows], axis=0), spread, precision=HIGHEST
    )
    tail_gb = wide[tokens : 2 * tokens] * gb
    x = big[:, :width]
    upstream = g[...].astype(F32)
    d_act = wide[:tokens] * (u[:, :width] + tail_gb) + wide[2 * tokens : 2 * tokens + 1] * upstream
    d_pre = d_act * big[:, width : 2 * width]
    pre_out[:, :width] = d_pre
    cross = jnp.sum(gt[...].astype(F32) * s0[...].astype(F32), axis=0, keepdims=True)
    sums = dot(
        jnp.concatenate(
            [x * tail_gb, zg.astype(F32) * sc, jnp.broadcast_to(cross, (8, width))], axis=0
        ),
        gather,
        precision=HIGHEST,
    )
    e_part = sums[:tokens]
    c_part = sums[tokens : 2 * tokens]
    f_part = sums[2 * tokens : 2 * tokens + 1]
    row = lax.broadcasted_iota(jnp.int32, (tokens, tokens), 0)
    col = lax.broadcasted_iota(jnp.int32, (tokens, tokens), 1)
    col_part = dot((row == col).astype(F32), col_in[...], 1, 1, precision=HIGHEST)
    e_step = step * e_part
    d_total = row_in[...] + c_part - step * col_part - e_step
    at_end = jnp.sum(e_step, axis=0, keepdims=True) + small[2, tokens - 1 : tokens, :] * f_part
    d_decay = dot((row <= col).astype(F32), d_total, precision=HIGHEST) + at_end
    d_step = col_part + e_part - d_decay * jnp.exp(decay_log[...])
    step_out[...] = jnp.zeros_like(step_out)
    step_out[:, :heads] = (d_step * small[4]).astype(BF16)
    d_into = u[:, width : width + state_width] + dot(zs, gt[...], 1, 1)
    d_out_of = u[:, width + state_width :] + dot(zg, s0[...], 1, 1)
    slopes = 2 * width + mixed
    pre_out[:, width : width + state_width] = d_into * big[:, slopes : slopes + state_width]
    pre_out[:, width + state_width :] = d_out_of * big[:, slopes + state_width :]
    head_out[...] = pre_out[0:8, :]
    k_out[:, :width] = k_in[...]
    k_out[:, width:] = k_mix[...]


def conv_back_kernel(pre, ahead, step, kernel, out, mix_out, padded):
    tokens = pre.shape[0]
    width = out.shape[1] - 128
    padded[:tokens, :] = pre[...]
    padded[tokens:, :] = ahead[...]

    def convolved(lanes):
        total = kernel[3:4, lanes] * padded[:tokens, lanes]
        for k in range(3):
            total = total + kernel[k : k + 1, lanes] * padded[3 - k : 3 - k + tokens, lanes]
        return total

    out[:, :width] = convolved(slice(0, width)).astype(BF16)
    out[:, width:] = step[...]
    mix_out[...] = convolved(slice(width, pre.shape[1])).astype(BF16)


def input_grad_kernel(who, grads, mix_grads, w_mix, w_step, w_in, *refs):
    outs, whole = refs[:4], refs[4]
    width = w_in.shape[1]
    heads = w_step.shape[0]
    total = dot(grads[:, :width], w_in[...], 1, 1)
    total = total + dot(mix_grads[...], w_mix[...], 1, 1)
    total = total + dot(grads[:, width : width + heads], w_step[...])
    whole[...] = total.astype(BF16)
    part = outs[0].shape[0]
    for k, out in enumerate(outs):
        slot = lax.rem(who[0] + k, 4)
        out[...] = whole[pl.ds(pl.multiple_of(slot * part, 16), part), :]


def pair_add_kernel(a, b, out):
    out[...] = (a[...].astype(F32) + b[...].astype(F32)).astype(BF16)


def add_kernel(m0, m1, m2, m3, out):
    total = m0[...].astype(F32) + m1[...].astype(F32) + m2[...].astype(F32) + m3[...].astype(F32)
    out[...] = total.astype(BF16)


def gathered_product(slabs, grads):
    total = None
    for k, grad in enumerate(grads):
        part = dot(slabs[k // 2][k % 2], grad[...])
        total = part if total is None else total + part
    return total


def inner_weight_kernel(*refs):
    refs[-1][...] = gathered_product(refs[:4], refs[4:12]).astype(BF16)


def mixer_weight_kernel(who, *refs):
    slabs, grads, inner, out = refs[:4], refs[4:12], refs[12], refs[13]
    chan = who[0]
    lines, share, _ = out.shape
    total = gathered_product(slabs, grads).astype(BF16)
    few = share // 4
    to_row = lax.broadcasted_iota(jnp.int32, (share, 4 * share), 0)
    source = lax.broadcasted_iota(jnp.int32, (share, 4 * share), 1)
    group = to_row // few
    wanted = group * share + chan * few + (to_row - group * few)
    pick = (source == wanted).astype(BF16)
    edge = inner.shape[1] - 64
    out[:, :, :] = inner[...].reshape(out.shape)
    for line in range(lines):
        piece = total[line * share : (line + 1) * share, :]
        stacked = jnp.concatenate([piece[:, q * 64 : (q + 1) * 64] for q in range(4)], axis=0)
        out[line, :, edge:] = dot(pick, stacked).astype(BF16)


def total_kernel(terms, inner_out, mix_out, step_out, whole, *, norm):
    lines, share, _ = terms.shape
    width = inner_out.shape[1]
    few = share // 4
    total = terms[0].astype(F32)
    for k in range(1, lines):
        total = total + terms[k].astype(F32)
    whole[...] = total * norm
    inner_out[...] = whole[:, :width]
    edge = whole.shape[1] - 64
    for q in range(4):
        mix_out[:, q * 64 : (q + 1) * 64] = whole[q * few : (q + 1) * few, edge:]
    heads = step_out.shape[0]
    row = lax.broadcasted_iota(jnp.int32, (heads, 128), 0)
    col = lax.broadcasted_iota(jnp.int32, (heads, 128), 1)
    step_out[...] = dot(
        (row == col).astype(F32), whole[:, width : width + 128], 1, 1, precision=HIGHEST
    )


def a2a(value, axis):
    return lax.all_to_all(value, axis, split_axis=0, concat_axis=0, tiled=True)


def turned(value, axis, steps):
    count = lax.axis_size(axis)
    return lax.ppermute(value, axis, [(k, (k + steps) % count) for k in range(count)])


def layer(
    layer_input,
    inner_weight,
    mixer_weight,
    step_weight,
    conv_inner,
    conv_mixer,
    step_bias,
    decay_log,
    skip_gain,
    output_grad,
):
    own = layer_input[0]
    part, model = own.shape
    chans = lax.axis_size("chan")
    tokens = part * chans
    width = inner_weight.shape[1]
    heads = step_bias.shape[0]
    mixed = mixer_weight.shape[1]
    state_width = mixed // 2
    g = output_grad[0]
    who = jnp.stack(
        [lax.axis_index("chan"), lax.axis_index("seq_2"), lax.axis_index(ROW4)]
    ).astype(jnp.int32)
    bias = step_bias[None]
    rate = decay_log[None]
    skip = skip_gain[None]

    seq_count = lax.axis_size(SEQ)
    t, c = tokens, width

    arrived = []
    for k in (1, 2, 3):
        arrived.append(turned(own, "chan", k))
    tail_rows = own[part - 4 :]
    halos = [
        lax.ppermute(
            tail_rows,
            SEQ_CHAN,
            [(s * chans + chans - 1, (s + 1) * chans + k) for s in range(seq_count - 1)],
        )
        for k in range(chans)
    ]
    sources = [
        own, inner_weight, mixer_weight, step_weight.T, conv_inner, conv_mixer, bias, rate, g
    ]
    near = fetch(sources)
    x, big, z, small, rows, keep, send, kept = call(
        project_kernel,
        [
            ((t, model), BF16),
            ((t, 2 * c + 2 * mixed), F32),
            ((t, 2 * c), BF16),
            ((5, t, heads), F32),
            ((2, heads, t), F32),
            ((state_width, c + 128), F32),
            ((state_width, c + 128), BF16),
            ((state_width, c + 128), F32),
        ],
        [who, near[0], *arrived, *halos, *near[1:]],
        stores=(0, 1, 2, 3, 4, 7),
        scratch=[
            pltpu.VMEM((t + HALO, model), BF16),
            pltpu.VMEM((t + HALO, c), F32),
            pltpu.VMEM((t + HALO, mixed), F32),
        ],
        flops=700_000_000,
        early=True,
    )
    got = turned(send, "seq_2", 1)
    groups = lax.axis_size(PAIRS)
    per = state_width // groups
    (pairs,) = call(pair_kernel, [((groups, per, c + 128), BF16)], [keep, got])
    pairs = a2a(pairs, PAIRS)

    u, row_part, col_part = call(
        within_kernel,
        [((t, c + mixed), F32), ((t, heads), F32), ((heads, t), F32)],
        [big, g, small, rows],
        loads=(0, 1, 2, 3),
        stores=(0, 1, 2),
        flops=700_000_000,
    )
    share = model // lax.axis_size(DP_SEQ)
    lines = lax.axis_size("seq_0")
    slab_shape = (lines * share, t)
    slab_keep, slab_send = call(
        lambda *refs: pack_kernel(*refs, half=lax.axis_size("seq_1")),
        [((4, *slab_shape), BF16)] * 2,
        [who, x],
        loads=(1,),
        stores=(0, 1),
        scratch=[pltpu.VMEM((model, t), F32)],
        flops=500_000_000,
    )
    slab_got = turned(slab_send, "seq_2", 1)
    slabs = call(
        join_kernel,
        [((2, *slab_shape), BF16)] * 4,
        [slab_keep, slab_got],
        loads=(0,),
        stores=(0,),
        flops=500_000_000,
    )
    far, close, next_close = [turned(slabs[k], ROW4, k) for k in (2, 1, 3)]
    slabs = fetch([slabs[0], close, far, next_close])

    (befores,) = call(
        chain_kernel,
        [((groups, per, c), BF16)],
        [who, pairs],
        scratch=[pltpu.VMEM((groups, c), F32)],
    )
    befores = a2a(befores, PAIRS)
    mine, others = call(back_kernel, [((state_width, c), BF16)] * 2, [kept, befores], loads=(0,))
    others = turned(others, "seq_2", 1)
    sources = [big, z, small, u, row_part, col_part, g, rate, skip, conv_inner, conv_mixer]
    fetched = fetch(sources, after=mine)
    pre, head, step_grad, kernels = call(
        back_through_kernel,
        [((t, c + mixed), F32), ((8, c + mixed), F32), ((t, 128), BF16), ((4, c + mixed), F32)],
        [who, mine, others, *fetched],
        scratch=[pltpu.VMEM((state_width, c), BF16), pltpu.VMEM((state_width, c), BF16)],
        flops=500_000_000,
    )
    ahead = lax.ppermute(head, SEQ, [(k + 1, k) for k in range(seq_count - 1)])
    grads, mix_grads = call(
        conv_back_kernel,
        [((t, c + 128), BF16), ((t, mixed), BF16)],
        [pre, ahead, step_grad, kernels],
        scratch=[pltpu.VMEM((t + 8, c + mixed), F32)],
    )
    far, near, next_near = [turned(grads, ROW4, k) for k in (2, 1, 3)]
    same = [grads, near, far, next_near]
    mix_total = mix_grads
    for partners in ([1, 0, 3, 2], [3, 2, 1, 0]):
        theirs = lax.ppermute(mix_total, "chan", list(enumerate(partners)))
        (mix_total,) = call(pair_add_kernel, [((t, mixed), BF16)], [mix_total, theirs])
    far, near, next_near = [turned(mix_total, ROW4, k) for k in (2, 1, 3)]
    mix_same = [mix_total, near, far, next_near]
    swapped = [turned(v, "seq_2", 1) for v in same]
    mix_swapped = [turned(v, "seq_2", 1) for v in mix_same]
    partial = call(
        input_grad_kernel,
        [((part, model), BF16)] * chans,
        [who, grads, mix_grads, mixer_weight, step_weight.T, inner_weight],
        stores=(0, 1, 2, 3),
        scratch=[pltpu.VMEM((tokens, model), BF16)],
        flops=500_000_000,
    )
    partial = [partial[0]] + [turned(partial[k], "chan", k) for k in (2, 1, 3)]
    (input_grad,) = call(add_kernel, [((part, model), BF16)], partial)
    (inner_terms,) = call(
        inner_weight_kernel,
        [((lines * share, c + 128), BF16)],
        [*slabs, *[v for pair in zip(same, swapped) for v in pair]],
        flops=700_000_000,
    )
    (terms,) = call(
        mixer_weight_kernel,
        [((lines, share, c + 128), BF16)],
        [who, *slabs, *[v for pair in zip(mix_same, mix_swapped) for v in pair], inner_terms],
        flops=700_000_000,
    )
    norm = 1.0 / math.sqrt(tokens * seq_count * lax.axis_size("dp"))
    terms = a2a(terms, "seq_0")
    inner_weight_grad, mixer_weight_grad, step_weight_grad = call(
        lambda *refs: total_kernel(*refs, norm=norm),
        [((share, c), F32), ((share // chans, mixed), F32), ((heads, share), F32)],
        [terms],
        scratch=[pltpu.VMEM((share, c + 128), F32)],
    )
    return input_grad[None], inner_weight_grad, mixer_weight_grad, step_weight_grad.T


def solution(mesh):
    split = Mesh(
        mesh.devices.reshape(mesh.shape["dp"], 8, 2, 2, mesh.shape["chan"]),
        ("dp", "seq_0", "seq_1", "seq_2", "chan"),
    )
    placed = (
        P("dp", SEQ_CHAN, None),
        P(None, "chan"),
        P(),
        P(None, "chan"),
        P(None, "chan"),
        P(),
        P("chan"),
        P("chan"),
        P("chan"),
        P("dp", SEQ, "chan"),
    )
    return jax.shard_map(
        layer,
        mesh=split,
        in_specs=placed,
        out_specs=(
            P("dp", SEQ_CHAN, None),
            P(DP_SEQ, "chan"),
            P(DP_SEQ_CHAN, None),
            P(DP_SEQ, "chan"),
        ),
        check_vma=False,
    )
```

```python
import math

import jax
import jax.numpy as jnp
from jax import lax
from jax.experimental import pallas as pl
from jax.experimental.pallas import tpu as pltpu
from jax.sharding import Mesh
from jax.sharding import PartitionSpec as P


HDIM = 64
SEQ = ("seq_0", "seq_1", "seq_2")
PAIRS = ("seq_0", "seq_1")
ROW4 = ("dp", "seq_1")
DP_SEQ = ("dp", "seq_0", "seq_1", "seq_2")
SEQ_CHAN = ("seq_0", "seq_1", "seq_2", "chan")
DP_SEQ_CHAN = ("dp", "seq_0", "seq_1", "seq_2", "chan")

F32 = jnp.float32
BF16 = jnp.bfloat16
HIGHEST = lax.Precision.HIGHEST
HALO = 16


def dot(a, b, ca=1, cb=0, precision=None):
    return lax.dot_general(
        a, b, (((ca,), (cb,)), ((), ())), precision=precision, preferred_element_type=F32
    )


def in_hbm(value):
    return pltpu.with_memory_space_constraint(value, pltpu.HBM)


def call(kernel, outs, ins, loads=(), stores=(), far=(), scratch=(), flops=0, early=False):
    count = len(ins)

    def wrapped(*refs):
        refs = list(refs)
        operands, results = refs[:count], refs[count : count + len(outs)]
        spare = refs[count + len(outs) :]
        sems = spare.pop()
        copies = []
        for k, position in enumerate(loads):
            buffer = spare.pop(0)
            copies.append(pltpu.make_async_copy(operands[position], buffer, sems.at[k]))
            operands[position] = buffer
        for copy in copies:
            copy.start()
        pending = {}
        for k, position in enumerate(stores):
            buffer = spare.pop(0)
            pending[position] = pltpu.make_async_copy(
                buffer, results[position], sems.at[len(loads) + k]
            )
            results[position] = buffer
        for copy in copies:
            copy.wait()
        started = []

        def flush(position):
            pending[position].start()
            started.append(position)

        if early:
            kernel(*operands, *results, *spare, flush=flush)
        else:
            kernel(*operands, *results, *spare)
        for position in stores:
            if position not in started:
                pending[position].start()
        for position in stores:
            pending[position].wait()

    specs, values = [], []
    for k, a in enumerate(ins):
        space = pltpu.VMEM
        if a.dtype == jnp.int32:
            space = pltpu.SMEM
        elif k in loads or k in far:
            space = pltpu.HBM
            a = in_hbm(a)
        specs.append(pl.BlockSpec(memory_space=space))
        values.append(a)
    buffers = [pltpu.VMEM(ins[k].shape, ins[k].dtype) for k in loads]
    buffers += [pltpu.VMEM(*outs[k]) for k in stores]
    return pl.pallas_call(
            wrapped,
            out_shape=[
                pltpu.HBM(s, d) if k in stores else jax.ShapeDtypeStruct(s, d)
                for k, (s, d) in enumerate(outs)
            ],
            in_specs=specs,
            out_specs=[
                pl.BlockSpec(memory_space=pltpu.HBM if k in stores else pltpu.VMEM)
                for k in range(len(outs))
            ],
            scratch_shapes=buffers
            + list(scratch)
            + [pltpu.SemaphoreType.DMA((len(loads) + len(stores) + 1,))],
            compiler_params=pltpu.CompilerParams(vmem_limit_bytes=24 << 20),
            cost_estimate=pl.CostEstimate(flops=flops, transcendentals=0, bytes_accessed=1 << 20),
    )(*values)


def fetch(values, after=None):
    count = len(values)

    def kernel(*refs):
        sources, outs, sems = refs[:count], refs[-1 - count : -1], refs[-1]
        copies = [
            pltpu.make_async_copy(source, out, sems.at[k])
            for k, (source, out) in enumerate(zip(sources, outs))
        ]
        for copy in copies:
            copy.start()
        for copy in copies:
            copy.wait()

    extra = [] if after is None else [after]
    return pl.pallas_call(
        kernel,
        out_shape=[jax.ShapeDtypeStruct(v.shape, v.dtype) for v in values],
        in_specs=[pl.BlockSpec(memory_space=pltpu.HBM)] * count
        + [pl.BlockSpec(memory_space=pltpu.VMEM)] * len(extra),
        out_specs=[pl.BlockSpec(memory_space=pltpu.VMEM)] * count,
        scratch_shapes=[pltpu.SemaphoreType.DMA((count,))],
        compiler_params=pltpu.CompilerParams(vmem_limit_bytes=16 << 20),
        cost_estimate=pl.CostEstimate(flops=700_000_000, transcendentals=0, bytes_accessed=4 << 20),
    )(*[in_hbm(v) for v in values], *extra)


def heads_to_lanes(heads, width):
    head = lax.broadcasted_iota(jnp.int32, (heads, width), 0)
    lane = lax.broadcasted_iota(jnp.int32, (heads, width), 1)
    return (lane // HDIM == head).astype(F32)


def lanes_to_heads(width, heads):
    lane = lax.broadcasted_iota(jnp.int32, (width, heads), 0)
    head = lax.broadcasted_iota(jnp.int32, (width, heads), 1)
    return (lane // HDIM == head).astype(F32)


def lower(size):
    row = lax.broadcasted_iota(jnp.int32, (size, size), 0)
    col = lax.broadcasted_iota(jnp.int32, (size, size), 1)
    return row >= col


def silu_and_slope(v):
    gate = 1.0 / (1.0 + jnp.exp(-v))
    return v * gate, gate * (1.0 + v * (1.0 - gate))


def project_kernel(
    who, x0, x1, x2, x3, h0, h1, h2, h3, w_in, w_mix, w_step, k_in, k_mix, bias, decay_log, g,
    x_out, big, z_out, small, rows, keep, send, kept,
    xs, pi, pm, *, flush,
):
    chan, core = who[0], who[1]
    part = x0.shape[0]
    tokens = 4 * part
    width = k_in.shape[1]
    mixed = k_mix.shape[1]
    state_width = mixed // 2
    heads = bias.shape[1]
    for k, x in enumerate((x0, x1, x2, x3)):
        slot = lax.rem(chan + 4 - k, 4)
        xs[pl.ds(pl.multiple_of(HALO + slot * part, 16), part), :] = x[...]
    edge = h0.shape[0]
    xs[0:HALO, :] = jnp.zeros_like(xs[0:HALO, :])
    xs[0:edge, :] = h0[...] + h1[...] + h2[...] + h3[...]
    everything = xs[...]
    x_out[...] = xs[HALO:, :]
    flush(0)
    pi[...] = dot(everything, w_in[...]).astype(BF16).astype(F32)
    pm[...] = dot(everything, w_mix[...]).astype(BF16).astype(F32)
    pi[HALO - edge : HALO, :] = pi[0:edge, :]
    pm[HALO - edge : HALO, :] = pm[0:edge, :]
    raw = dot(xs[HALO:, :], w_step[...], 1, 1) + bias[...]

    def convolved(source, kernel):
        total = kernel[3:4, :] * source[HALO:, :]
        for k in range(3):
            start = HALO - 3 + k
            total = total + kernel[k : k + 1, :] * source[start : start + tokens, :]
        return total

    inner_act, inner_slope = silu_and_slope(convolved(pi, k_in))
    big[:, :width] = inner_act.astype(BF16)
    big[:, width : 2 * width] = inner_slope.astype(BF16)
    mix_act, mixer_slope = silu_and_slope(convolved(pm, k_mix))
    big[:, 2 * width : 2 * width + mixed] = mix_act.astype(BF16)
    big[:, 2 * width + mixed :] = mixer_slope.astype(BF16)
    flush(1)

    step = jnp.maximum(raw, 0.0) + jnp.log1p(jnp.exp(-jnp.abs(raw)))
    decay = -step * jnp.exp(decay_log[...])
    low = lower(tokens).astype(F32)
    total = dot(low, decay, precision=HIGHEST)
    rows[0] = dot(decay, low, 0, 1, precision=HIGHEST)
    row = lax.broadcasted_iota(jnp.int32, (tokens, tokens), 0)
    col = lax.broadcasted_iota(jnp.int32, (tokens, tokens), 1)
    rows[1] = dot(step, (row == col).astype(F32), 0, 0, precision=HIGHEST)
    last = total[tokens - 1 : tokens, :]
    ea = jnp.exp(total)
    tail = jnp.exp(last - total)
    small[0] = step
    small[1] = total
    small[2] = ea
    small[3] = tail
    small[4] = 1.0 / (1.0 + jnp.exp(-raw))
    spread = heads_to_lanes(heads, width)
    wide = dot(jnp.concatenate([tail * step, ea], axis=0), spread, precision=HIGHEST)
    zs = (wide[:tokens] * inner_act).astype(BF16)
    zg = (wide[tokens:] * g[...].astype(F32)).astype(BF16)
    z_out[:, :width] = zs
    z_out[:, width:] = zg
    for k in (2, 3, 4):
        flush(k)
    into = mix_act[:, :state_width].astype(BF16)
    out_of = mix_act[:, state_width:].astype(BF16)
    state = dot(into, zs, 0, 0)
    grad = dot(out_of, zg, 0, 0)
    lead = last.astype(BF16)
    keep[:, width:] = jnp.zeros_like(keep[:, width:])
    send[:, width:] = jnp.zeros_like(send[:, width:])
    keep[0:1, width : width + heads] = last
    send[0:1, width : width + heads] = lead
    send[1:2, width : width + heads] = (last - lead.astype(F32)).astype(BF16)

    @pl.when(core == 0)
    def _():
        keep[:, :width] = state
        send[:, :width] = grad.astype(BF16)

    @pl.when(core != 0)
    def _():
        keep[:, :width] = grad
        send[:, :width] = state.astype(BF16)

    kept[...] = keep[...]


def pair_kernel(keep, recv, out):
    groups, per = out.shape[0], out.shape[1]
    heads = out.shape[2] // HDIM - 2
    width = heads * HDIM
    spread = heads_to_lanes(heads, width)
    own = keep[0:8, width : width + heads]
    other = recv[0:16, width : width + heads].astype(F32)
    theirs = other[0:1] + other[1:2]
    wide = dot(jnp.broadcast_to(jnp.exp(theirs), (8, heads)), spread, precision=HIGHEST)
    pair = (wide[0:1] * keep[:, :width] + recv[:, :width].astype(F32)).astype(BF16)
    total = own[0:1] + theirs
    lead = total.astype(BF16)
    rest = (total - lead.astype(F32)).astype(BF16)
    out[:, :, :width] = pair.reshape(groups, per, width)
    out[:, :, width:] = jnp.zeros_like(out[:, :, width:])
    for k in range(groups):
        out[k, 0:1, width : width + heads] = lead
        out[k, 1:2, width : width + heads] = rest


def chain_kernel(who, recv, out, factors):
    forward = who[1] == 0
    groups = recv.shape[0]
    width = out.shape[2]
    heads = width // HDIM
    marks = recv[:, 0, width : width + heads].astype(F32)
    marks = marks + recv[:, 1, width : width + heads].astype(F32)
    factors[...] = dot(jnp.exp(marks), heads_to_lanes(heads, width), precision=HIGHEST)

    def step(k, state):
        slot = jnp.where(forward, k, groups - 1 - k)
        out[slot] = state.astype(BF16)
        return factors[pl.ds(slot, 1), :] * state + recv[slot, :, :width].astype(F32)

    lax.fori_loop(0, groups, step, jnp.zeros(out.shape[1:], F32), unroll=True)


def back_kernel(keep, before, own, send):
    groups, per, width = before.shape
    heads = width // HDIM
    last = jnp.broadcast_to(keep[0:1, width : width + heads], (8, heads))
    factor = dot(jnp.exp(last), heads_to_lanes(heads, width), precision=HIGHEST)[0:1]
    piece = before[...].reshape(groups * per, width)
    own[...] = piece
    send[...] = (factor * piece.astype(F32) + keep[:, :width]).astype(BF16)


def pack_kernel(who, x, keep, send, turned_x, *, half):
    core, place = who[1], who[2]
    model = x.shape[1]
    lines = 8
    share = keep.shape[1] // lines
    for k in range(model // 128):
        lanes = slice(k * 128, (k + 1) * 128)
        turned_x[lanes, :] = x[:, lanes].astype(F32).T
    for out, side in ((keep, core), (send, 1 - core)):
        for steps in range(4):
            where = lax.rem(place + steps, 4)
            outer = where // half
            inner = 2 * (where - outer * half) + side
            for line in range(lines):
                start = share * ((outer * lines + line) * 2 * half + inner)
                out[steps, line * share : (line + 1) * share, :] = turned_x[
                    pl.ds(pl.multiple_of(start, 8), share), :
                ].astype(BF16)


def join_kernel(keep, got, *outs):
    for k, out in enumerate(outs):
        out[0] = keep[k]
        out[1] = got[k]


def within_kernel(big, g, small, rows, u_out, row_out, col_out):
    tokens, width = g.shape
    mixed = (big.shape[1] - 2 * width) // 2
    state_width = mixed // 2
    into = big[:, 2 * width : 2 * width + state_width]
    out_of = big[:, 2 * width + state_width : 2 * width + mixed]
    scores = dot(out_of, into, 1, 1)
    causal = lower(tokens)
    lane = lax.broadcasted_iota(jnp.int32, (tokens, 128), 1)
    pull = jnp.zeros((tokens, tokens), F32)
    for pair in range(width // 128):
        lanes = slice(pair * 128, (pair + 1) * 128)
        x_pair = big[:, lanes]
        g_pair = g[:, lanes]
        u_pair = jnp.zeros((tokens, 128), F32)
        for half in range(2):
            h = 2 * pair + half
            g_head = jnp.where(lane // HDIM == half, g_pair, jnp.zeros_like(g_pair))
            inner = dot(g_head, x_pair, 1, 1)
            spread = small[1, :, h : h + 1] - rows[0, h : h + 1, :]
            decay = jnp.where(causal, jnp.exp(jnp.where(causal, spread, 0.0)), 0.0)
            weights = decay * scores
            u_pair = u_pair + dot(weights.astype(BF16), g_head, 0, 0)
            step_row = rows[1, h : h + 1, :]
            both = weights * inner
            col_out[h : h + 1, :] = jnp.sum(both, axis=0, keepdims=True)
            row_out[:, h : h + 1] = jnp.sum(both * step_row, axis=1, keepdims=True)
            pull = pull + decay * inner * step_row
        u_out[:, lanes] = u_pair
    pull = pull.astype(BF16)
    u_out[:, width : width + state_width] = dot(pull, out_of, 0, 0)
    u_out[:, width + state_width :] = dot(pull, into)


def back_through_kernel(
    who, own, other, big, z, small, u, row_in, col_in, g, decay_log, skip, k_in, k_mix,
    pre_out, head_out, step_out, k_out, s0, gt,
):
    tokens, width = g.shape
    heads = small.shape[2]
    mixed = (big.shape[1] - 2 * width) // 2
    state_width = mixed // 2

    @pl.when(who[1] == 0)
    def _():
        s0[...] = own[...]
        gt[...] = other[...]

    @pl.when(who[1] != 0)
    def _():
        s0[...] = other[...]
        gt[...] = own[...]

    into = big[:, 2 * width : 2 * width + state_width]
    out_of = big[:, 2 * width + state_width : 2 * width + mixed]
    zs = z[:, :width]
    zg = z[:, width:]
    gb = dot(into, gt[...])
    sc = dot(out_of, s0[...])
    step = small[0]
    spread = heads_to_lanes(heads, width)
    gather = lanes_to_heads(width, heads)
    skip_rows = jnp.broadcast_to(skip[...], (8, heads))
    wide = dot(
        jnp.concatenate([step, small[3], skip_rows], axis=0), spread, precision=HIGHEST
    )
    tail_gb = wide[tokens : 2 * tokens] * gb
    x = big[:, :width].astype(F32)
    upstream = g[...].astype(F32)
    d_act = wide[:tokens] * (u[:, :width] + tail_gb) + wide[2 * tokens : 2 * tokens + 1] * upstream
    d_pre = d_act * big[:, width : 2 * width].astype(F32)
    pre_out[:, :width] = d_pre
    cross = jnp.sum(gt[...].astype(F32) * s0[...].astype(F32), axis=0, keepdims=True)
    sums = dot(
        jnp.concatenate(
            [x * tail_gb, zg.astype(F32) * sc, jnp.broadcast_to(cross, (8, width))], axis=0
        ),
        gather,
        precision=HIGHEST,
    )
    e_part = sums[:tokens]
    c_part = sums[tokens : 2 * tokens]
    f_part = sums[2 * tokens : 2 * tokens + 1]
    row = lax.broadcasted_iota(jnp.int32, (tokens, tokens), 0)
    col = lax.broadcasted_iota(jnp.int32, (tokens, tokens), 1)
    col_part = dot((row == col).astype(F32), col_in[...], 1, 1, precision=HIGHEST)
    e_step = step * e_part
    d_total = row_in[...] + c_part - step * col_part - e_step
    at_end = jnp.sum(e_step, axis=0, keepdims=True) + small[2, tokens - 1 : tokens, :] * f_part
    d_decay = dot((row <= col).astype(F32), d_total, precision=HIGHEST) + at_end
    d_step = col_part + e_part - d_decay * jnp.exp(decay_log[...])
    step_out[...] = jnp.zeros_like(step_out)
    step_out[:, :heads] = (d_step * small[4]).astype(BF16)
    d_into = u[:, width : width + state_width] + dot(zs, gt[...], 1, 1)
    d_out_of = u[:, width + state_width :] + dot(zg, s0[...], 1, 1)
    slopes = 2 * width + mixed
    pre_out[:, width : width + state_width] = d_into * big[:, slopes : slopes + state_width].astype(F32)
    pre_out[:, width + state_width :] = d_out_of * big[:, slopes + state_width :].astype(F32)
    head_out[...] = pre_out[0:8, :]
    k_out[:, :width] = k_in[...]
    k_out[:, width:] = k_mix[...]


def conv_back_kernel(pre, ahead, step, kernel, out, mix_out, padded):
    tokens = pre.shape[0]
    width = out.shape[1] - 128
    padded[:tokens, :] = pre[...]
    padded[tokens:, :] = ahead[...]

    def convolved(lanes):
        total = kernel[3:4, lanes] * padded[:tokens, lanes]
        for k in range(3):
            total = total + kernel[k : k + 1, lanes] * padded[3 - k : 3 - k + tokens, lanes]
        return total

    out[:, :width] = convolved(slice(0, width)).astype(BF16)
    out[:, width:] = step[...]
    mix_out[...] = convolved(slice(width, pre.shape[1])).astype(BF16)


def input_grad_kernel(who, grads, mix_grads, w_mix, w_step, w_in, *refs):
    outs, whole = refs[:4], refs[4]
    width = w_in.shape[1]
    heads = w_step.shape[0]
    total = dot(grads[:, :width], w_in[...], 1, 1)
    total = total + dot(mix_grads[...], w_mix[...], 1, 1)
    total = total + dot(grads[:, width : width + heads], w_step[...])
    whole[...] = total.astype(BF16)
    part = outs[0].shape[0]
    for k, out in enumerate(outs):
        slot = lax.rem(who[0] + k, 4)
        out[...] = whole[pl.ds(pl.multiple_of(slot * part, 16), part), :]


def pair_add_kernel(a, b, out):
    out[...] = (a[...].astype(F32) + b[...].astype(F32)).astype(BF16)


def add_kernel(m0, m1, m2, m3, out):
    total = m0[...].astype(F32) + m1[...].astype(F32) + m2[...].astype(F32) + m3[...].astype(F32)
    out[...] = total.astype(BF16)


def gathered_product(slabs, grads):
    total = None
    for k, grad in enumerate(grads):
        part = dot(slabs[k // 2][k % 2], grad[...])
        total = part if total is None else total + part
    return total


def inner_weight_kernel(*refs):
    refs[-1][...] = gathered_product(refs[:4], refs[4:12]).astype(BF16)


def mixer_weight_kernel(who, *refs):
    slabs, grads, inner, out = refs[:4], refs[4:12], refs[12], refs[13]
    chan = who[0]
    lines, share, _ = out.shape
    total = gathered_product(slabs, grads).astype(BF16)
    few = share // 4
    to_row = lax.broadcasted_iota(jnp.int32, (share, 4 * share), 0)
    source = lax.broadcasted_iota(jnp.int32, (share, 4 * share), 1)
    group = to_row // few
    wanted = group * share + chan * few + (to_row - group * few)
    pick = (source == wanted).astype(BF16)
    edge = inner.shape[1] - 64
    out[:, :, :] = inner[...].reshape(out.shape)
    for line in range(lines):
        piece = total[line * share : (line + 1) * share, :]
        stacked = jnp.concatenate([piece[:, q * 64 : (q + 1) * 64] for q in range(4)], axis=0)
        out[line, :, edge:] = dot(pick, stacked).astype(BF16)


def total_kernel(terms, inner_out, mix_out, step_out, whole, *, norm):
    lines, share, _ = terms.shape
    width = inner_out.shape[1]
    few = share // 4
    total = terms[0].astype(F32)
    for k in range(1, lines):
        total = total + terms[k].astype(F32)
    whole[...] = total * norm
    inner_out[...] = whole[:, :width]
    edge = whole.shape[1] - 64
    for q in range(4):
        mix_out[:, q * 64 : (q + 1) * 64] = whole[q * few : (q + 1) * few, edge:]
    heads = step_out.shape[0]
    row = lax.broadcasted_iota(jnp.int32, (heads, 128), 0)
    col = lax.broadcasted_iota(jnp.int32, (heads, 128), 1)
    step_out[...] = dot(
        (row == col).astype(F32), whole[:, width : width + 128], 1, 1, precision=HIGHEST
    )


def a2a(value, axis):
    return lax.all_to_all(value, axis, split_axis=0, concat_axis=0, tiled=True)


def turned(value, axis, steps):
    count = lax.axis_size(axis)
    return lax.ppermute(value, axis, [(k, (k + steps) % count) for k in range(count)])


def layer(
    layer_input,
    inner_weight,
    mixer_weight,
    step_weight,
    conv_inner,
    conv_mixer,
    step_bias,
    decay_log,
    skip_gain,
    output_grad,
):
    own = layer_input[0]
    part, model = own.shape
    chans = lax.axis_size("chan")
    tokens = part * chans
    width = inner_weight.shape[1]
    heads = step_bias.shape[0]
    mixed = mixer_weight.shape[1]
    state_width = mixed // 2
    g = output_grad[0]
    who = jnp.stack(
        [lax.axis_index("chan"), lax.axis_index("seq_2"), lax.axis_index(ROW4)]
    ).astype(jnp.int32)
    bias = step_bias[None]
    rate = decay_log[None]
    skip = skip_gain[None]

    seq_count = lax.axis_size(SEQ)
    t, c = tokens, width

    arrived = []
    for k in (1, 2, 3):
        arrived.append(turned(own, "chan", k))
    tail_rows = own[part - 4 :]
    halos = [
        lax.ppermute(
            tail_rows,
            SEQ_CHAN,
            [(s * chans + chans - 1, (s + 1) * chans + k) for s in range(seq_count - 1)],
        )
        for k in range(chans)
    ]
    sources = [
        own, inner_weight, mixer_weight, step_weight.T, conv_inner, conv_mixer, bias, rate, g
    ]
    near = fetch(sources)
    x, big, z, small, rows, keep, send, kept = call(
        project_kernel,
        [
            ((t, model), BF16),
            ((t, 2 * c + 2 * mixed), BF16),
            ((t, 2 * c), BF16),
            ((5, t, heads), F32),
            ((2, heads, t), F32),
            ((state_width, c + 128), F32),
            ((state_width, c + 128), BF16),
            ((state_width, c + 128), F32),
        ],
        [who, near[0], *arrived, *halos, *near[1:]],
        stores=(0, 1, 2, 3, 4, 7),
        scratch=[
            pltpu.VMEM((t + HALO, model), BF16),
            pltpu.VMEM((t + HALO, c), F32),
            pltpu.VMEM((t + HALO, mixed), F32),
        ],
        flops=700_000_000,
        early=True,
    )
    got = turned(send, "seq_2", 1)
    groups = lax.axis_size(PAIRS)
    per = state_width // groups
    (pairs,) = call(pair_kernel, [((groups, per, c + 128), BF16)], [keep, got])
    pairs = a2a(pairs, PAIRS)

    u, row_part, col_part = call(
        within_kernel,
        [((t, c + mixed), F32), ((t, heads), F32), ((heads, t), F32)],
        [big, g, small, rows],
        loads=(0, 1, 2, 3),
        stores=(0, 1, 2),
        flops=700_000_000,
    )
    share = model // lax.axis_size(DP_SEQ)
    lines = lax.axis_size("seq_0")
    slab_shape = (lines * share, t)
    slab_keep, slab_send = call(
        lambda *refs: pack_kernel(*refs, half=lax.axis_size("seq_1")),
        [((4, *slab_shape), BF16)] * 2,
        [who, x],
        loads=(1,),
        stores=(0, 1),
        scratch=[pltpu.VMEM((model, t), F32)],
        flops=500_000_000,
    )
    slab_got = turned(slab_send, "seq_2", 1)
    slabs = call(
        join_kernel,
        [((2, *slab_shape), BF16)] * 4,
        [slab_keep, slab_got],
        loads=(0,),
        stores=(0,),
        flops=500_000_000,
    )
    far, close, next_close = [turned(slabs[k], ROW4, k) for k in (2, 1, 3)]
    slabs = fetch([slabs[0], close, far, next_close])

    (befores,) = call(
        chain_kernel,
        [((groups, per, c), BF16)],
        [who, pairs],
        scratch=[pltpu.VMEM((groups, c), F32)],
    )
    befores = a2a(befores, PAIRS)
    mine, others = call(back_kernel, [((state_width, c), BF16)] * 2, [kept, befores], loads=(0,))
    others = turned(others, "seq_2", 1)
    sources = [big, z, small, u, row_part, col_part, g, rate, skip, conv_inner, conv_mixer]
    fetched = fetch(sources, after=mine)
    pre, head, step_grad, kernels = call(
        back_through_kernel,
        [((t, c + mixed), F32), ((8, c + mixed), F32), ((t, 128), BF16), ((4, c + mixed), F32)],
        [who, mine, others, *fetched],
        scratch=[pltpu.VMEM((state_width, c), BF16), pltpu.VMEM((state_width, c), BF16)],
        flops=500_000_000,
    )
    ahead = lax.ppermute(head, SEQ, [(k + 1, k) for k in range(seq_count - 1)])
    grads, mix_grads = call(
        conv_back_kernel,
        [((t, c + 128), BF16), ((t, mixed), BF16)],
        [pre, ahead, step_grad, kernels],
        scratch=[pltpu.VMEM((t + 8, c + mixed), F32)],
    )
    far, near, next_near = [turned(grads, ROW4, k) for k in (2, 1, 3)]
    same = [grads, near, far, next_near]
    mix_total = mix_grads
    for partners in ([1, 0, 3, 2], [3, 2, 1, 0]):
        theirs = lax.ppermute(mix_total, "chan", list(enumerate(partners)))
        (mix_total,) = call(pair_add_kernel, [((t, mixed), BF16)], [mix_total, theirs])
    far, near, next_near = [turned(mix_total, ROW4, k) for k in (2, 1, 3)]
    mix_same = [mix_total, near, far, next_near]
    swapped = [turned(v, "seq_2", 1) for v in same]
    mix_swapped = [turned(v, "seq_2", 1) for v in mix_same]
    partial = call(
        input_grad_kernel,
        [((part, model), BF16)] * chans,
        [who, grads, mix_grads, mixer_weight, step_weight.T, inner_weight],
        stores=(0, 1, 2, 3),
        scratch=[pltpu.VMEM((tokens, model), BF16)],
        flops=500_000_000,
    )
    partial = [partial[0]] + [turned(partial[k], "chan", k) for k in (2, 1, 3)]
    (input_grad,) = call(add_kernel, [((part, model), BF16)], partial)
    (inner_terms,) = call(
        inner_weight_kernel,
        [((lines * share, c + 128), BF16)],
        [*slabs, *[v for pair in zip(same, swapped) for v in pair]],
        flops=700_000_000,
    )
    (terms,) = call(
        mixer_weight_kernel,
        [((lines, share, c + 128), BF16)],
        [who, *slabs, *[v for pair in zip(mix_same, mix_swapped) for v in pair], inner_terms],
        flops=700_000_000,
    )
    norm = 1.0 / math.sqrt(tokens * seq_count * lax.axis_size("dp"))
    terms = a2a(terms, "seq_0")
    inner_weight_grad, mixer_weight_grad, step_weight_grad = call(
        lambda *refs: total_kernel(*refs, norm=norm),
        [((share, c), F32), ((share // chans, mixed), F32), ((heads, share), F32)],
        [terms],
        scratch=[pltpu.VMEM((share, c + 128), F32)],
    )
    return input_grad[None], inner_weight_grad, mixer_weight_grad, step_weight_grad.T


def solution(mesh):
    split = Mesh(
        mesh.devices.reshape(mesh.shape["dp"], 8, 2, 2, mesh.shape["chan"]),
        ("dp", "seq_0", "seq_1", "seq_2", "chan"),
    )
    placed = (
        P("dp", SEQ_CHAN, None),
        P(None, "chan"),
        P(),
        P(None, "chan"),
        P(None, "chan"),
        P(),
        P("chan"),
        P("chan"),
        P("chan"),
        P("dp", SEQ, "chan"),
    )
    return jax.shard_map(
        layer,
        mesh=split,
        in_specs=placed,
        out_specs=(
            P("dp", SEQ_CHAN, None),
            P(DP_SEQ, "chan"),
            P(DP_SEQ_CHAN, None),
            P(DP_SEQ, "chan"),
        ),
        check_vma=False,
    )
```

```python
import math

import jax
import jax.numpy as jnp
from jax import lax
from jax.experimental import pallas as pl
from jax.experimental.pallas import tpu as pltpu
from jax.sharding import Mesh
from jax.sharding import PartitionSpec as P


HDIM = 64
SEQ = ("seq_0", "seq_1", "seq_2")
PAIRS = ("seq_0", "seq_1")
ROW4 = ("dp", "seq_1")
DP_SEQ = ("dp", "seq_0", "seq_1", "seq_2")
SEQ_CHAN = ("seq_0", "seq_1", "seq_2", "chan")
DP_SEQ_CHAN = ("dp", "seq_0", "seq_1", "seq_2", "chan")

F32 = jnp.float32
BF16 = jnp.bfloat16
HIGHEST = lax.Precision.HIGHEST
HALO = 16


def dot(a, b, ca=1, cb=0, precision=None):
    return lax.dot_general(
        a, b, (((ca,), (cb,)), ((), ())), precision=precision, preferred_element_type=F32
    )


def in_hbm(value):
    return pltpu.with_memory_space_constraint(value, pltpu.HBM)


def call(kernel, outs, ins, loads=(), stores=(), far=(), scratch=(), flops=0, early=False):
    count = len(ins)

    def wrapped(*refs):
        refs = list(refs)
        operands, results = refs[:count], refs[count : count + len(outs)]
        spare = refs[count + len(outs) :]
        sems = spare.pop()
        copies = []
        for k, position in enumerate(loads):
            buffer = spare.pop(0)
            copies.append(pltpu.make_async_copy(operands[position], buffer, sems.at[k]))
            operands[position] = buffer
        for copy in copies:
            copy.start()
        pending = {}
        for k, position in enumerate(stores):
            buffer = spare.pop(0)
            pending[position] = pltpu.make_async_copy(
                buffer, results[position], sems.at[len(loads) + k]
            )
            results[position] = buffer
        for copy in copies:
            copy.wait()
        started = []

        def flush(position):
            pending[position].start()
            started.append(position)

        if early:
            kernel(*operands, *results, *spare, flush=flush)
        else:
            kernel(*operands, *results, *spare)
        for position in stores:
            if position not in started:
                pending[position].start()
        for position in stores:
            pending[position].wait()

    specs, values = [], []
    for k, a in enumerate(ins):
        space = pltpu.VMEM
        if a.dtype == jnp.int32:
            space = pltpu.SMEM
        elif k in loads or k in far:
            space = pltpu.HBM
            a = in_hbm(a)
        specs.append(pl.BlockSpec(memory_space=space))
        values.append(a)
    buffers = [pltpu.VMEM(ins[k].shape, ins[k].dtype) for k in loads]
    buffers += [pltpu.VMEM(*outs[k]) for k in stores]
    return pl.pallas_call(
            wrapped,
            out_shape=[
                pltpu.HBM(s, d) if k in stores else jax.ShapeDtypeStruct(s, d)
                for k, (s, d) in enumerate(outs)
            ],
            in_specs=specs,
            out_specs=[
                pl.BlockSpec(memory_space=pltpu.HBM if k in stores else pltpu.VMEM)
                for k in range(len(outs))
            ],
            scratch_shapes=buffers
            + list(scratch)
            + [pltpu.SemaphoreType.DMA((len(loads) + len(stores) + 1,))],
            compiler_params=pltpu.CompilerParams(vmem_limit_bytes=24 << 20),
            cost_estimate=pl.CostEstimate(flops=flops, transcendentals=0, bytes_accessed=1 << 20),
    )(*values)


def fetch(values, after=None):
    count = len(values)

    def kernel(*refs):
        sources, outs, sems = refs[:count], refs[-1 - count : -1], refs[-1]
        copies = [
            pltpu.make_async_copy(source, out, sems.at[k])
            for k, (source, out) in enumerate(zip(sources, outs))
        ]
        for copy in copies:
            copy.start()
        for copy in copies:
            copy.wait()

    extra = [] if after is None else [after]
    return pl.pallas_call(
        kernel,
        out_shape=[jax.ShapeDtypeStruct(v.shape, v.dtype) for v in values],
        in_specs=[pl.BlockSpec(memory_space=pltpu.HBM)] * count
        + [pl.BlockSpec(memory_space=pltpu.VMEM)] * len(extra),
        out_specs=[pl.BlockSpec(memory_space=pltpu.VMEM)] * count,
        scratch_shapes=[pltpu.SemaphoreType.DMA((count,))],
        compiler_params=pltpu.CompilerParams(vmem_limit_bytes=16 << 20),
        cost_estimate=pl.CostEstimate(flops=700_000_000, transcendentals=0, bytes_accessed=4 << 20),
    )(*[in_hbm(v) for v in values], *extra)


def heads_to_lanes(heads, width):
    head = lax.broadcasted_iota(jnp.int32, (heads, width), 0)
    lane = lax.broadcasted_iota(jnp.int32, (heads, width), 1)
    return (lane // HDIM == head).astype(F32)


def lanes_to_heads(width, heads):
    lane = lax.broadcasted_iota(jnp.int32, (width, heads), 0)
    head = lax.broadcasted_iota(jnp.int32, (width, heads), 1)
    return (lane // HDIM == head).astype(F32)


def lower(size):
    row = lax.broadcasted_iota(jnp.int32, (size, size), 0)
    col = lax.broadcasted_iota(jnp.int32, (size, size), 1)
    return row >= col


def silu_and_slope(v):
    gate = 1.0 / (1.0 + jnp.exp(-v))
    return v * gate, gate * (1.0 + v * (1.0 - gate))


def project_kernel(
    who, x0, x1, x2, x3, h0, h1, h2, h3, w_in, w_mix, w_step, k_in, k_mix, bias, decay_log, g,
    x_out, big, z_out, small, rows, keep, send, kept,
    xs, pi, pm, *, flush,
):
    chan, core = who[0], who[1]
    part = x0.shape[0]
    tokens = 4 * part
    width = k_in.shape[1]
    mixed = k_mix.shape[1]
    state_width = mixed // 2
    heads = bias.shape[1]
    for k, x in enumerate((x0, x1, x2, x3)):
        slot = lax.rem(chan + 4 - k, 4)
        xs[pl.ds(pl.multiple_of(HALO + slot * part, 16), part), :] = x[...]
    edge = h0.shape[0]
    xs[0:HALO, :] = jnp.zeros_like(xs[0:HALO, :])
    xs[0:edge, :] = h0[...] + h1[...] + h2[...] + h3[...]
    everything = xs[...]
    x_out[...] = xs[HALO:, :]
    flush(0)
    pi[...] = dot(everything, w_in[...]).astype(BF16).astype(F32)
    pm[...] = dot(everything, w_mix[...]).astype(BF16).astype(F32)
    pi[HALO - edge : HALO, :] = pi[0:edge, :]
    pm[HALO - edge : HALO, :] = pm[0:edge, :]
    raw = dot(xs[HALO:, :], w_step[...], 1, 1) + bias[...]

    def convolved(source, kernel):
        total = kernel[3:4, :] * source[HALO:, :]
        for k in range(3):
            start = HALO - 3 + k
            total = total + kernel[k : k + 1, :] * source[start : start + tokens, :]
        return total

    inner_act, inner_slope = silu_and_slope(convolved(pi, k_in))
    big[:, :width] = inner_act
    big[:, width : 2 * width] = inner_slope
    mix_act, mixer_slope = silu_and_slope(convolved(pm, k_mix))
    big[:, 2 * width : 2 * width + mixed] = mix_act
    big[:, 2 * width + mixed :] = mixer_slope
    flush(1)

    step = jnp.maximum(raw, 0.0) + jnp.log1p(jnp.exp(-jnp.abs(raw)))
    decay = -step * jnp.exp(decay_log[...])
    low = lower(tokens).astype(F32)
    total = dot(low, decay, precision=HIGHEST)
    rows[0] = dot(decay, low, 0, 1, precision=HIGHEST)
    row = lax.broadcasted_iota(jnp.int32, (tokens, tokens), 0)
    col = lax.broadcasted_iota(jnp.int32, (tokens, tokens), 1)
    rows[1] = dot(step, (row == col).astype(F32), 0, 0, precision=HIGHEST)
    last = total[tokens - 1 : tokens, :]
    ea = jnp.exp(total)
    tail = jnp.exp(last - total)
    small[0] = step
    small[1] = total
    small[2] = ea
    small[3] = tail
    small[4] = 1.0 / (1.0 + jnp.exp(-raw))
    spread = heads_to_lanes(heads, width)
    wide = dot(jnp.concatenate([tail * step, ea], axis=0), spread, precision=HIGHEST)
    zs = (wide[:tokens] * inner_act).astype(BF16)
    zg = (wide[tokens:] * g[...].astype(F32)).astype(BF16)
    z_out[:, :width] = zs
    z_out[:, width:] = zg
    for k in (2, 3, 4):
        flush(k)
    into = mix_act[:, :state_width].astype(BF16)
    out_of = mix_act[:, state_width:].astype(BF16)
    state = dot(into, zs, 0, 0)
    grad = dot(out_of, zg, 0, 0)
    lead = last.astype(BF16)
    keep[:, width:] = jnp.zeros_like(keep[:, width:])
    send[:, width:] = jnp.zeros_like(send[:, width:])
    keep[0:1, width : width + heads] = last
    send[0:1, width : width + heads] = lead
    send[1:2, width : width + heads] = (last - lead.astype(F32)).astype(BF16)

    @pl.when(core == 0)
    def _():
        keep[:, :width] = state
        send[:, :width] = grad.astype(BF16)

    @pl.when(core != 0)
    def _():
        keep[:, :width] = grad
        send[:, :width] = state.astype(BF16)

    kept[...] = keep[...]


def pair_kernel(keep, recv, out):
    groups, per = out.shape[0], out.shape[1]
    heads = out.shape[2] // HDIM - 2
    width = heads * HDIM
    spread = heads_to_lanes(heads, width)
    own = keep[0:8, width : width + heads]
    other = recv[0:16, width : width + heads].astype(F32)
    theirs = other[0:1] + other[1:2]
    wide = dot(jnp.broadcast_to(jnp.exp(theirs), (8, heads)), spread, precision=HIGHEST)
    pair = (wide[0:1] * keep[:, :width] + recv[:, :width].astype(F32)).astype(BF16)
    total = own[0:1] + theirs
    lead = total.astype(BF16)
    rest = (total - lead.astype(F32)).astype(BF16)
    out[:, :, :width] = pair.reshape(groups, per, width)
    out[:, :, width:] = jnp.zeros_like(out[:, :, width:])
    for k in range(groups):
        out[k, 0:1, width : width + heads] = lead
        out[k, 1:2, width : width + heads] = rest


def chain_kernel(who, recv, out, factors):
    forward = who[1] == 0
    groups = recv.shape[0]
    width = out.shape[2]
    heads = width // HDIM
    marks = recv[:, 0, width : width + heads].astype(F32)
    marks = marks + recv[:, 1, width : width + heads].astype(F32)
    factors[...] = dot(jnp.exp(marks), heads_to_lanes(heads, width), precision=HIGHEST)

    def step(k, state):
        slot = jnp.where(forward, k, groups - 1 - k)
        out[slot] = state.astype(BF16)
        return factors[pl.ds(slot, 1), :] * state + recv[slot, :, :width].astype(F32)

    lax.fori_loop(0, groups, step, jnp.zeros(out.shape[1:], F32), unroll=True)


def back_kernel(keep, before, own, send):
    groups, per, width = before.shape
    heads = width // HDIM
    last = jnp.broadcast_to(keep[0:1, width : width + heads], (8, heads))
    factor = dot(jnp.exp(last), heads_to_lanes(heads, width), precision=HIGHEST)[0:1]
    piece = before[...].reshape(groups * per, width)
    own[...] = piece
    send[...] = (factor * piece.astype(F32) + keep[:, :width]).astype(BF16)


def pack_kernel(who, x, keep, send, turned_x, *, half):
    core, place = who[1], who[2]
    model = x.shape[1]
    lines = 8
    share = keep.shape[1] // lines
    for k in range(model // 128):
        lanes = slice(k * 128, (k + 1) * 128)
        turned_x[lanes, :] = x[:, lanes].astype(F32).T
    for out, side in ((keep, core), (send, 1 - core)):
        for steps in range(4):
            where = lax.rem(place + steps, 4)
            outer = where // half
            inner = 2 * (where - outer * half) + side
            for line in range(lines):
                start = share * ((outer * lines + line) * 2 * half + inner)
                out[steps, line * share : (line + 1) * share, :] = turned_x[
                    pl.ds(pl.multiple_of(start, 8), share), :
                ].astype(BF16)


def join_kernel(keep, got, *outs):
    for k, out in enumerate(outs):
        out[0] = keep[k]
        out[1] = got[k]


def within_kernel(big, g, small, rows, u_out, row_out, col_out):
    tokens, width = g.shape
    mixed = (big.shape[1] - 2 * width) // 2
    state_width = mixed // 2
    into = big[:, 2 * width : 2 * width + state_width].astype(BF16)
    out_of = big[:, 2 * width + state_width : 2 * width + mixed].astype(BF16)
    scores = dot(out_of, into, 1, 1)
    causal = lower(tokens)
    lane = lax.broadcasted_iota(jnp.int32, (tokens, 128), 1)
    pull = jnp.zeros((tokens, tokens), F32)
    for pair in range(width // 128):
        lanes = slice(pair * 128, (pair + 1) * 128)
        x_pair = big[:, lanes].astype(BF16)
        g_pair = g[:, lanes]
        u_pair = jnp.zeros((tokens, 128), F32)
        for half in range(2):
            h = 2 * pair + half
            g_head = jnp.where(lane // HDIM == half, g_pair, jnp.zeros_like(g_pair))
            inner = dot(g_head, x_pair, 1, 1)
            spread = small[1, :, h : h + 1] - rows[0, h : h + 1, :]
            decay = jnp.where(causal, jnp.exp(jnp.where(causal, spread, 0.0)), 0.0)
            weights = decay * scores
            u_pair = u_pair + dot(weights.astype(BF16), g_head, 0, 0)
            step_row = rows[1, h : h + 1, :]
            both = weights * inner
            col_out[h : h + 1, :] = jnp.sum(both, axis=0, keepdims=True)
            row_out[:, h : h + 1] = jnp.sum(both * step_row, axis=1, keepdims=True)
            pull = pull + decay * inner * step_row
        u_out[:, lanes] = u_pair
    pull = pull.astype(BF16)
    u_out[:, width : width + state_width] = dot(pull, out_of, 0, 0)
    u_out[:, width + state_width :] = dot(pull, into)


def back_through_kernel(
    who, own, other, big, z, small, u, row_in, col_in, g, decay_log, skip, k_in, k_mix,
    pre_out, head_out, step_out, k_out, s0, gt,
):
    tokens, width = g.shape
    heads = small.shape[2]
    mixed = (big.shape[1] - 2 * width) // 2
    state_width = mixed // 2

    @pl.when(who[1] == 0)
    def _():
        s0[...] = own[...]
        gt[...] = other[...]

    @pl.when(who[1] != 0)
    def _():
        s0[...] = other[...]
        gt[...] = own[...]

    into = big[:, 2 * width : 2 * width + state_width].astype(BF16)
    out_of = big[:, 2 * width + state_width : 2 * width + mixed].astype(BF16)
    zs = z[:, :width]
    zg = z[:, width:]
    gb = dot(into, gt[...])
    sc = dot(out_of, s0[...])
    step = small[0]
    spread = heads_to_lanes(heads, width)
    gather = lanes_to_heads(width, heads)
    skip_rows = jnp.broadcast_to(skip[...], (8, heads))
    wide = dot(
        jnp.concatenate([step, small[3], skip_rows], axis=0), spread, precision=HIGHEST
    )
    tail_gb = wide[tokens : 2 * tokens] * gb
    x = big[:, :width]
    upstream = g[...].astype(F32)
    d_act = wide[:tokens] * (u[:, :width] + tail_gb) + wide[2 * tokens : 2 * tokens + 1] * upstream
    d_pre = d_act * big[:, width : 2 * width]
    pre_out[:, :width] = d_pre
    cross = jnp.sum(gt[...].astype(F32) * s0[...].astype(F32), axis=0, keepdims=True)
    sums = dot(
        jnp.concatenate(
            [x * tail_gb, zg.astype(F32) * sc, jnp.broadcast_to(cross, (8, width))], axis=0
        ),
        gather,
        precision=HIGHEST,
    )
    e_part = sums[:tokens]
    c_part = sums[tokens : 2 * tokens]
    f_part = sums[2 * tokens : 2 * tokens + 1]
    row = lax.broadcasted_iota(jnp.int32, (tokens, tokens), 0)
    col = lax.broadcasted_iota(jnp.int32, (tokens, tokens), 1)
    col_part = dot((row == col).astype(F32), col_in[...], 1, 1, precision=HIGHEST)
    e_step = step * e_part
    d_total = row_in[...] + c_part - step * col_part - e_step
    at_end = jnp.sum(e_step, axis=0, keepdims=True) + small[2, tokens - 1 : tokens, :] * f_part
    d_decay = dot((row <= col).astype(F32), d_total, precision=HIGHEST) + at_end
    d_step = col_part + e_part - d_decay * jnp.exp(decay_log[...])
    step_out[...] = jnp.zeros_like(step_out)
    step_out[:, :heads] = (d_step * small[4]).astype(BF16)
    d_into = u[:, width : width + state_width] + dot(zs, gt[...], 1, 1)
    d_out_of = u[:, width + state_width :] + dot(zg, s0[...], 1, 1)
    slopes = 2 * width + mixed
    pre_out[:, width : width + state_width] = d_into * big[:, slopes : slopes + state_width]
    pre_out[:, width + state_width :] = d_out_of * big[:, slopes + state_width :]
    head_out[...] = pre_out[0:8, :]
    k_out[:, :width] = k_in[...]
    k_out[:, width:] = k_mix[...]


def conv_back_kernel(pre, ahead, step, kernel, out, mix_out, padded):
    tokens = pre.shape[0]
    width = out.shape[1] - 128
    padded[:tokens, :] = pre[...]
    padded[tokens:, :] = ahead[...]

    def convolved(lanes):
        total = kernel[3:4, lanes] * padded[:tokens, lanes]
        for k in range(3):
            total = total + kernel[k : k + 1, lanes] * padded[3 - k : 3 - k + tokens, lanes]
        return total

    out[:, :width] = convolved(slice(0, width)).astype(BF16)
    out[:, width:] = step[...]
    mix_out[...] = convolved(slice(width, pre.shape[1])).astype(BF16)


def input_grad_kernel(who, grads, mix_grads, w_mix, w_step, w_in, *refs):
    outs, whole = refs[:4], refs[4]
    width = w_in.shape[1]
    heads = w_step.shape[0]
    total = dot(grads[:, :width], w_in[...], 1, 1)
    total = total + dot(mix_grads[...], w_mix[...], 1, 1)
    total = total + dot(grads[:, width : width + heads], w_step[...])
    whole[...] = total.astype(BF16)
    part = outs[0].shape[0]
    for k, out in enumerate(outs):
        slot = lax.rem(who[0] + k, 4)
        out[...] = whole[pl.ds(pl.multiple_of(slot * part, 16), part), :]


def pair_add_kernel(a, b, out):
    out[...] = (a[...].astype(F32) + b[...].astype(F32)).astype(BF16)


def add_kernel(m0, m1, m2, m3, out):
    total = m0[...].astype(F32) + m1[...].astype(F32) + m2[...].astype(F32) + m3[...].astype(F32)
    out[...] = total.astype(BF16)


def gathered_product(slabs, grads):
    total = None
    for k, grad in enumerate(grads):
        part = dot(slabs[k // 2][k % 2], grad[...])
        total = part if total is None else total + part
    return total


def inner_weight_kernel(*refs):
    refs[-1][...] = gathered_product(refs[:4], refs[4:12]).astype(BF16)


def mixer_weight_kernel(who, *refs):
    slabs, grads, inner, out = refs[:4], refs[4:12], refs[12], refs[13]
    chan = who[0]
    lines, share, _ = out.shape
    total = gathered_product(slabs, grads).astype(BF16)
    few = share // 4
    to_row = lax.broadcasted_iota(jnp.int32, (share, 4 * share), 0)
    source = lax.broadcasted_iota(jnp.int32, (share, 4 * share), 1)
    group = to_row // few
    wanted = group * share + chan * few + (to_row - group * few)
    pick = (source == wanted).astype(BF16)
    edge = inner.shape[1] - 64
    out[:, :, :] = inner[...].reshape(out.shape)
    for line in range(lines):
        piece = total[line * share : (line + 1) * share, :]
        stacked = jnp.concatenate([piece[:, q * 64 : (q + 1) * 64] for q in range(4)], axis=0)
        out[line, :, edge:] = dot(pick, stacked).astype(BF16)


def total_kernel(terms, inner_out, mix_out, step_out, whole, *, norm):
    lines, share, _ = terms.shape
    width = inner_out.shape[1]
    few = share // 4
    total = terms[0].astype(F32)
    for k in range(1, lines):
        total = total + terms[k].astype(F32)
    whole[...] = total * norm
    inner_out[...] = whole[:, :width]
    edge = whole.shape[1] - 64
    for q in range(4):
        mix_out[:, q * 64 : (q + 1) * 64] = whole[q * few : (q + 1) * few, edge:]
    heads = step_out.shape[0]
    row = lax.broadcasted_iota(jnp.int32, (heads, 128), 0)
    col = lax.broadcasted_iota(jnp.int32, (heads, 128), 1)
    step_out[...] = dot(
        (row == col).astype(F32), whole[:, width : width + 128], 1, 1, precision=HIGHEST
    )


def a2a(value, axis):
    return lax.all_to_all(value, axis, split_axis=0, concat_axis=0, tiled=True)


def turned(value, axis, steps):
    count = lax.axis_size(axis)
    return lax.ppermute(value, axis, [(k, (k + steps) % count) for k in range(count)])


def layer(
    layer_input,
    inner_weight,
    mixer_weight,
    step_weight,
    conv_inner,
    conv_mixer,
    step_bias,
    decay_log,
    skip_gain,
    output_grad,
):
    own = layer_input[0]
    part, model = own.shape
    chans = lax.axis_size("chan")
    tokens = part * chans
    width = inner_weight.shape[1]
    heads = step_bias.shape[0]
    mixed = mixer_weight.shape[1]
    state_width = mixed // 2
    g = output_grad[0]
    who = jnp.stack(
        [lax.axis_index("chan"), lax.axis_index("seq_2"), lax.axis_index(ROW4)]
    ).astype(jnp.int32)
    bias = step_bias[None]
    rate = decay_log[None]
    skip = skip_gain[None]

    seq_count = lax.axis_size(SEQ)
    t, c = tokens, width

    arrived = []
    for k in (1, 2, 3):
        arrived.append(turned(own, "chan", k))
    tail_rows = own[part - 4 :]
    halos = []
    for k in range(chans):
        halos.append(
            lax.ppermute(
                tail_rows,
                SEQ_CHAN,
                [(s * chans + chans - 1, (s + 1) * chans + k) for s in range(seq_count - 1)],
            )
        )
    sources = [
        own, inner_weight, mixer_weight, step_weight.T, conv_inner, conv_mixer, bias, rate, g
    ]
    near = fetch(sources)
    x, big, z, small, rows, keep, send, kept = call(
        project_kernel,
        [
            ((t, model), BF16),
            ((t, 2 * c + 2 * mixed), F32),
            ((t, 2 * c), BF16),
            ((5, t, heads), F32),
            ((2, heads, t), F32),
            ((state_width, c + 128), F32),
            ((state_width, c + 128), BF16),
            ((state_width, c + 128), F32),
        ],
        [who, near[0], *arrived, *halos, *near[1:]],
        stores=(0, 1, 2, 3, 4, 7),
        scratch=[
            pltpu.VMEM((t + HALO, model), BF16),
            pltpu.VMEM((t + HALO, c), F32),
            pltpu.VMEM((t + HALO, mixed), F32),
        ],
        flops=700_000_000,
        early=True,
    )
    got = turned(send, "seq_2", 1)
    groups = lax.axis_size(PAIRS)
    per = state_width // groups
    (pairs,) = call(pair_kernel, [((groups, per, c + 128), BF16)], [keep, got])
    pairs = a2a(pairs, PAIRS)

    u, row_part, col_part = call(
        within_kernel,
        [((t, c + mixed), F32), ((t, heads), F32), ((heads, t), F32)],
        [big, g, small, rows],
        loads=(0, 1, 2, 3),
        stores=(0, 1, 2),
        flops=700_000_000,
    )
    share = model // lax.axis_size(DP_SEQ)
    lines = lax.axis_size("seq_0")
    slab_shape = (lines * share, t)
    slab_keep, slab_send = call(
        lambda *refs: pack_kernel(*refs, half=lax.axis_size("seq_1")),
        [((4, *slab_shape), BF16)] * 2,
        [who, x],
        loads=(1,),
        stores=(0, 1),
        scratch=[pltpu.VMEM((model, t), F32)],
        flops=500_000_000,
    )
    slab_got = turned(slab_send, "seq_2", 1)
    slabs = call(
        join_kernel,
        [((2, *slab_shape), BF16)] * 4,
        [slab_keep, slab_got],
        loads=(0,),
        stores=(0,),
        flops=500_000_000,
    )
    far, close, next_close = [turned(slabs[k], ROW4, k) for k in (2, 1, 3)]
    slabs = fetch([slabs[0], close, far, next_close])

    (befores,) = call(
        chain_kernel,
        [((groups, per, c), BF16)],
        [who, pairs],
        scratch=[pltpu.VMEM((groups, c), F32)],
    )
    befores = a2a(befores, PAIRS)
    mine, others = call(back_kernel, [((state_width, c), BF16)] * 2, [kept, befores], loads=(0,))
    others = turned(others, "seq_2", 1)
    sources = [big, z, small, u, row_part, col_part, g, rate, skip, conv_inner, conv_mixer]
    fetched = fetch(sources, after=mine)
    pre, head, step_grad, kernels = call(
        back_through_kernel,
        [((t, c + mixed), F32), ((8, c + mixed), F32), ((t, 128), BF16), ((4, c + mixed), F32)],
        [who, mine, others, *fetched],
        scratch=[pltpu.VMEM((state_width, c), BF16), pltpu.VMEM((state_width, c), BF16)],
        flops=500_000_000,
    )
    ahead = lax.ppermute(head, SEQ, [(k + 1, k) for k in range(seq_count - 1)])
    grads, mix_grads = call(
        conv_back_kernel,
        [((t, c + 128), BF16), ((t, mixed), BF16)],
        [pre, ahead, step_grad, kernels],
        scratch=[pltpu.VMEM((t + 8, c + mixed), F32)],
    )
    far, near, next_near = [turned(grads, ROW4, k) for k in (2, 1, 3)]
    same = [grads, near, far, next_near]
    mix_total = mix_grads
    for partners in ([1, 0, 3, 2], [3, 2, 1, 0]):
        theirs = lax.ppermute(mix_total, "chan", list(enumerate(partners)))
        (mix_total,) = call(pair_add_kernel, [((t, mixed), BF16)], [mix_total, theirs])
    far, near, next_near = [turned(mix_total, ROW4, k) for k in (2, 1, 3)]
    mix_same = [mix_total, near, far, next_near]
    swapped = [turned(v, "seq_2", 1) for v in same]
    mix_swapped = [turned(v, "seq_2", 1) for v in mix_same]
    partial = call(
        input_grad_kernel,
        [((part, model), BF16)] * chans,
        [who, grads, mix_grads, mixer_weight, step_weight.T, inner_weight],
        stores=(0, 1, 2, 3),
        scratch=[pltpu.VMEM((tokens, model), BF16)],
        flops=500_000_000,
    )
    partial = [partial[0]] + [turned(partial[k], "chan", k) for k in (2, 1, 3)]
    (input_grad,) = call(add_kernel, [((part, model), BF16)], partial)
    (inner_terms,) = call(
        inner_weight_kernel,
        [((lines * share, c + 128), BF16)],
        [*slabs, *[v for pair in zip(same, swapped) for v in pair]],
        flops=700_000_000,
    )
    (terms,) = call(
        mixer_weight_kernel,
        [((lines, share, c + 128), BF16)],
        [who, *slabs, *[v for pair in zip(mix_same, mix_swapped) for v in pair], inner_terms],
        flops=700_000_000,
    )
    norm = 1.0 / math.sqrt(tokens * seq_count * lax.axis_size("dp"))
    terms = a2a(terms, "seq_0")
    inner_weight_grad, mixer_weight_grad, step_weight_grad = call(
        lambda *refs: total_kernel(*refs, norm=norm),
        [((share, c), F32), ((share // chans, mixed), F32), ((heads, share), F32)],
        [terms],
        scratch=[pltpu.VMEM((share, c + 128), F32)],
    )
    return input_grad[None], inner_weight_grad, mixer_weight_grad, step_weight_grad.T


def solution(mesh):
    split = Mesh(
        mesh.devices.reshape(mesh.shape["dp"], 8, 2, 2, mesh.shape["chan"]),
        ("dp", "seq_0", "seq_1", "seq_2", "chan"),
    )
    placed = (
        P("dp", SEQ_CHAN, None),
        P(None, "chan"),
        P(),
        P(None, "chan"),
        P(None, "chan"),
        P(),
        P("chan"),
        P("chan"),
        P("chan"),
        P("dp", SEQ, "chan"),
    )
    return jax.shard_map(
        layer,
        mesh=split,
        in_specs=placed,
        out_specs=(
            P("dp", SEQ_CHAN, None),
            P(DP_SEQ, "chan"),
            P(DP_SEQ_CHAN, None),
            P(DP_SEQ, "chan"),
        ),
        check_vma=False,
    )
```
